256 devices in a mesh: dp: 64 (over x, z, core), mp: 4 (over y).
Axes of the slice: x: 4, y: 4, z: 8, core: 2. Of those that a mesh axis runs over, the one named last changes fastest.
Arguments:
- queries: bfloat16 [128, 16, 5120], P('dp', None, 'mp')
- key_value_cache: bfloat16 [3072, 2, 128, 1024], P('dp', None, None, 'mp'), may hold values from -6 to 6
- slot_tags: int32 [3072], P('dp'), may hold values from 0 to 127, as said below
- span_key_value: bfloat16 [128, 2, 16, 1024], P('dp', None, None, 'mp'), may hold values from -6 to 6
- answer_id: int32 [128], P('dp'), may hold values from 0 to 127
- w_cand: bfloat16 [5120, 128], P('mp')
Outputs:
- attended: bfloat16 [128, 16, 5120], P('dp', None, 'mp')
- chain_score: float32 [128], P('dp')
- answer_tally: float32 [8, 128], P(None, 'dp')
The draws below stay inside these ranges and needn't reach their ends.
Inputs may be any that keep to these rules, and one draw needn't show every extreme that they name: `slot_tags`: among the 48 blocks of any one index of dp, at most 2 belong to the chains o * 2 to o * 2 + 1 of any one o, and for some o every index of dp holds exactly 2 such blocks. A chain may have no cached block.
All inputs are finite; a program needn't handle non-finite values.
Results may differ from the reference program's by a relative error of at most 0.0075.
Values may be sent and summed in bfloat16 or wider, within the bound.
A program may use at most 128 MiB of HBM per device.

```python
import jax
import jax.numpy as jnp
from jax import lax

QUERY_HEADS = 40
KEY_VALUE_HEADS = 8
HEAD_SIZE = 128
NCAND = 128
BLOCK_TOKENS = 128
ANSWER_TOKENS = 16
PEER = 2
SAMPLES = 16
CH_DEV = 2
SLOTS = 48
CHAIN_COUNT = 128
TOTAL_BLOCKS = 3072


def draw_queries(key, part):
    first = jax.random.fold_in(key, 0)
    base = jax.random.normal(first, (CHAIN_COUNT, ANSWER_TOKENS, QUERY_HEADS * HEAD_SIZE), jnp.float32)
    return base.astype(jnp.bfloat16)


def draw_w_cand(key, part):
    first = jax.random.fold_in(key, 0)
    base = jax.random.normal(first, (QUERY_HEADS * HEAD_SIZE, NCAND), jnp.float32) * (8.0 / (QUERY_HEADS * HEAD_SIZE) ** 0.5)
    return base.astype(jnp.bfloat16)


def draw_slot_tags(key, part):
    lookup_matrix = jax.random.split(jax.random.fold_in(key, 7), 5)
    accelerator_roster = CHAIN_COUNT // CH_DEV
    couple_sequence = accelerator_roster * PEER
    extra_credit = jax.random.randint(lookup_matrix[0], (accelerator_roster,), 0, 3)
    selected_reply = jax.random.randint(lookup_matrix[1], (), 0, accelerator_roster)
    extra_credit = jnp.where(jnp.arange(accelerator_roster) == selected_reply, 3, extra_credit)
    random_perturbation = jax.random.randint(lookup_matrix[2], (accelerator_roster, couple_sequence), 0, 4096)
    couple_container = jnp.arange(couple_sequence) // PEER
    sorted_permutation = (extra_credit[couple_container][None, :] * 4096 + random_perturbation) * couple_sequence + jnp.arange(couple_sequence)[None, :]
    order = jnp.argsort(-sorted_permutation, axis=1, stable=True)[:, :SLOTS]
    owners_of = order // PEER
    chain_pick = jax.random.randint(lookup_matrix[3], (accelerator_roster, SLOTS), 0, CH_DEV)
    tags_grid = owners_of * CH_DEV + chain_pick
    mixing = jax.random.randint(lookup_matrix[4], (accelerator_roster, SLOTS), 0, 1 << 20) * SLOTS + jnp.arange(SLOTS)[None, :]
    shuffle = jnp.argsort(mixing, axis=1, stable=True)
    tags_grid = jnp.take_along_axis(tags_grid, shuffle, axis=1)
    return tags_grid.reshape(accelerator_roster * SLOTS).astype(jnp.int32)


def place_ends(result, stream_key, smallest, top_value):
    longest = result.shape.index(max(result.shape))
    spots = []
    for shift in (0, 1):
        where = [jax.random.randint(jax.random.fold_in(stream_key, axis), (), 0, length) for axis, length in enumerate(result.shape)]
        where[longest] = (where[longest] + shift) % result.shape[longest]
        spots.append(tuple(where))
    return result.at[spots[0]].set(smallest).at[spots[1]].set(top_value)


def shard_levels(rng, extent, cuts, least, high):
    factor_of = 1.0
    for dim, blocks in cuts:
        steps = jax.random.uniform(jax.random.fold_in(jax.random.fold_in(rng, 6), dim), (blocks,), jnp.float32, least / len(cuts), high / len(cuts))
        factor_of = factor_of * jnp.repeat(jnp.exp(steps), extent[dim] // blocks).reshape((-1,) + (1,) * (len(extent) - 1 - dim))
    return factor_of


def bell_draw(rng, dims, deviation, bound, shards=(), kind=jnp.bfloat16):
    result = deviation * jax.random.normal(rng, dims, jnp.float32)
    if shards:
        result = result * shard_levels(rng, dims, shards, -0.22, 0.18)
    return jnp.clip(result, -bound, bound).astype(kind)


def setup_inputs(seed: int = 0) -> dict:
    seeds = jax.random.split(jax.random.key(seed), 7)
    queries = draw_queries(jax.random.fold_in(seeds[6], 71), 0)
    key_value_cache = bell_draw(seeds[1], (TOTAL_BLOCKS, 2, BLOCK_TOKENS, KEY_VALUE_HEADS * HEAD_SIZE), 1.0, 6.0, ((0, 64), (3, 4)))
    slot_tags = draw_slot_tags(jax.random.fold_in(seeds[6], 71), 0)
    span_key_value = bell_draw(seeds[3], (CHAIN_COUNT, 2, ANSWER_TOKENS, KEY_VALUE_HEADS * HEAD_SIZE), 1.0, 6.0, ((0, 64), (3, 4)))
    answer_id = place_ends(jax.random.randint(seeds[4], (CHAIN_COUNT,), 0, NCAND), jax.random.fold_in(seeds[4], 1), 0, NCAND - 1).astype(jnp.int32)
    w_cand = draw_w_cand(jax.random.fold_in(seeds[6], 71), 0)
    return {"queries": queries, "key_value_cache": key_value_cache, "slot_tags": slot_tags, "span_key_value": span_key_value, "answer_id": answer_id, "w_cand": w_cand}


big_neg = -1e30


def span_terms(single_queries, single_span):
    head_group = QUERY_HEADS // KEY_VALUE_HEADS
    query_rows = single_queries.astype(jnp.float32).reshape(ANSWER_TOKENS, KEY_VALUE_HEADS, head_group, HEAD_SIZE)
    lookup_matrix = single_span[0].astype(jnp.float32).reshape(ANSWER_TOKENS, KEY_VALUE_HEADS, HEAD_SIZE)
    value_rows = single_span[1].astype(jnp.float32).reshape(ANSWER_TOKENS, KEY_VALUE_HEADS, HEAD_SIZE)
    logit_rows = jnp.einsum('qufe,xue->ufqx', query_rows, lookup_matrix) * (HEAD_SIZE ** -0.5)
    causal = jnp.arange(ANSWER_TOKENS)[:, None] >= jnp.arange(ANSWER_TOKENS)[None, :]
    logit_rows = jnp.where(causal, logit_rows, big_neg)
    peak = jnp.max(logit_rows, axis=-1)
    weights = jnp.exp(logit_rows - peak[..., None])
    total = jnp.sum(weights, axis=-1)
    rounded_scores = lax.optimization_barrier(weights.astype(jnp.bfloat16))
    summed_scores = jnp.einsum('wefs,swn->wefn', rounded_scores.astype(jnp.float32), value_rows)
    return peak, total, summed_scores


def reference(queries, key_value_cache, slot_tags, span_key_value, answer_id, w_cand):
    head_group = QUERY_HEADS // KEY_VALUE_HEADS
    chains_all = queries.shape[0]
    peak, total, summed_scores = jax.vmap(span_terms)(queries, span_key_value)

    def absorb(carry, item):
        peak, total, summed_scores = carry
        current_tag, block_entry = item
        query_rows = queries[current_tag].astype(jnp.float32).reshape(ANSWER_TOKENS, KEY_VALUE_HEADS, head_group, HEAD_SIZE)
        lookup_matrix = block_entry[0].astype(jnp.float32).reshape(BLOCK_TOKENS, KEY_VALUE_HEADS, HEAD_SIZE)
        value_rows = block_entry[1].astype(jnp.float32).reshape(BLOCK_TOKENS, KEY_VALUE_HEADS, HEAD_SIZE)
        logit_rows = jnp.einsum('qufe,xue->ufqx', query_rows, lookup_matrix) * (HEAD_SIZE ** -0.5)
        older = peak[current_tag]
        fresh = jnp.maximum(older, jnp.max(logit_rows, axis=-1))
        weights = jnp.exp(logit_rows - fresh[..., None])
        shrink = jnp.exp(older - fresh)
        rounded_scores = lax.optimization_barrier(weights.astype(jnp.bfloat16))
        added_terms = jnp.einsum('wefs,swn->wefn', rounded_scores.astype(jnp.float32), value_rows)
        total = total.at[current_tag].set(total[current_tag] * shrink + jnp.sum(weights, axis=-1))
        summed_scores = summed_scores.at[current_tag].set(summed_scores[current_tag] * shrink[..., None] + added_terms)
        peak = peak.at[current_tag].set(fresh)
        return (peak, total, summed_scores), None

    (peak, total, summed_scores), _ = lax.scan(absorb, (peak, total, summed_scores), (slot_tags, key_value_cache))
    output = summed_scores / total[..., None]
    output = jnp.transpose(output, (0, 3, 1, 2, 4)).reshape(chains_all, ANSWER_TOKENS, QUERY_HEADS * HEAD_SIZE)
    attended = output.astype(jnp.bfloat16)
    logit_rows = jnp.dot(attended.reshape(chains_all * ANSWER_TOKENS, QUERY_HEADS * HEAD_SIZE), w_cand, preferred_element_type=jnp.float32)
    logit_rows = logit_rows.reshape(chains_all, ANSWER_TOKENS, NCAND)
    top_logit = jnp.max(logit_rows, axis=-1, keepdims=True)
    log_norm = top_logit[..., 0] + jnp.log(jnp.sum(jnp.exp(logit_rows - top_logit), axis=-1))
    answer_hot = (answer_id[:, None] == jnp.arange(NCAND, dtype=jnp.int32)[None, :]).astype(jnp.float32)
    picked = jnp.sum(logit_rows * answer_hot[:, None, :], axis=-1)
    chain_score = jnp.mean(picked - log_norm, axis=-1)
    prompt_of = jnp.arange(chains_all, dtype=jnp.int32) // SAMPLES
    prompt_hot = (prompt_of[:, None] == jnp.arange(chains_all // SAMPLES, dtype=jnp.int32)[None, :]).astype(jnp.float32)
    answer_tally = jnp.dot(prompt_hot.T, chain_score[:, None] * answer_hot, precision=lax.Precision.HIGHEST)
    return attended, chain_score, answer_tally
```

```python
import functools

import jax
import jax.numpy as jnp
from jax import lax
from jax.experimental import pallas as pl
from jax.experimental.pallas import tpu as pltpu
from jax.sharding import PartitionSpec as P

HEAD_SIZE = 128
NCAND = 128
SAMPLES = 16
SPAN = 16
GROUP = 5
ROWS = SPAN * GROUP
WIDE = GROUP * HEAD_SIZE
SLOTS = 48
EMPTY = SLOTS
OWN = SLOTS + 1
NX, NZ, NY = 4, 8, 4
big_neg = -1e30
SCALE = HEAD_SIZE ** (-0.5)
F32 = jnp.float32
BF16 = jnp.bfloat16

ARRIVALS = [
    (1, 0, 0), (0, 0, 0), (1, 0, -1), (1, 0, 1), (1, -1, 0), (1, 1, 0), (0, -1, 0), (0, 1, 0),
    (0, 0, -1), (0, 0, 1), (1, 0, -2), (1, -1, -1), (1, 1, -1), (1, 0, 2), (1, -1, 1), (1, 1, 1),
    (0, -1, -1), (0, -1, 1), (1, -2, 0), (0, 1, -1), (0, 1, 1), (0, -2, 0), (0, 0, -2), (0, 0, 2),
    (1, 1, -2), (1, 0, -3), (1, -1, -2), (1, 0, 3), (1, 1, 2), (1, -2, -1), (0, -1, -2), (0, -1, 2),
    (1, -1, 2), (0, 1, -2), (0, 1, 2), (1, -2, 1), (0, -2, -1), (0, -2, 1), (1, 1, -3), (0, 0, -3),
    (0, 0, 3), (1, -1, -3), (1, 1, 3), (1, 0, -4), (1, -2, -2), (0, -1, 3), (1, -1, 3), (0, -1, -3),
    (0, 1, 3), (1, -2, 2), (0, 1, -3), (0, -2, 2), (0, -2, -2), (1, -2, -3), (1, 1, -4), (0, 0, -4),
    (1, -1, -4), (1, -2, 3), (0, -1, -4), (0, -2, 3), (0, 1, -4), (0, -2, -3), (1, -2, -4), (0, -2, -4),
]
UNIT = {key: i for i, key in enumerate(ARRIVALS)}
MOVES = {"x+": (-1, 0), "x-": (1, 0), "z+": (0, -1), "z-": (0, 1)}


def onward(key):
    head, xr, zr = key
    out = []
    if head == 0 or xr == 0:
        if -4 < zr <= 0:
            out.append("z+")
        if 0 <= zr < 3:
            out.append("z-")
    if head == 1 or zr == 0:
        if -2 < xr <= 0:
            out.append("x+")
        if 0 <= xr < 1:
            out.append("x-")
    return out


STAGE1 = [(0, "L", k, 0) for k in (4, 3, 2, 1)] + [(0, "S", k, 0) for k in (3, 2, 1)]
STAGE1 += [(1, "L", k, half) for k in (2, 1) for half in (0, 1)] + [(1, "S", 1, half) for half in (0, 1)]
STAGE2 = [(0, "L", 2), (0, "L", 1), (0, "S", 1)]
STAGE2 += [(1, "L", k) for k in (4, 3, 2, 1)] + [(1, "S", k) for k in (3, 2, 1)]
MSG1 = {key: i for i, key in enumerate(STAGE1)}
MSG2 = {key: i for i, key in enumerate(STAGE2)}


def kernel(
    q_ref, idx_s, idx_v, ans_s, kv_hbm, span_ref, w_ref,
    att_ref, score_ref, tally_ref,
    g0, g1, kv, sbuf, res, dm, dl, spst, fscr,
    sib_s, sib_ss, sib_r, sib_rs, m1_s, m1_ss, m1_r, m1_rs, m2_s, m2_ss, m2_r, m2_rs,
    r0, r0s, r1, r1s, lg, tc, tx, tz,
    kv_sem, own_sem, ag_send, ag_recv, sg_send, sg_recv,
    sib_send, sib_recv, m1_send, m1_recv, m2_send, m2_recv, tail_send, tail_recv,
):
    dp = lax.axis_index("dp")
    y = lax.axis_index("mp")
    core = dp % 2
    z = (dp // 2) % NZ
    x = dp // (2 * NZ)
    s = 1 - 2 * core
    other = 1 - core

    def device(xx, zz, cc, yy):
        return (xx * (2 * NZ) + zz * 2 + cc, yy)

    def along_x(k):
        return (x + s * k + 2 * NX) % NX

    def along_z(k):
        return (z + s * k + 2 * NZ) % NZ

    sibling = device(x, z, other, y)
    link = {
        "x+": device(along_x(1), z, core, y),
        "x-": device(along_x(-1), z, core, y),
        "z+": device(x, along_z(1), core, y),
        "z-": device(x, along_z(-1), core, y),
    }
    started = []

    def send(src, dst, ssem, rsem, dev):
        copy = pltpu.make_async_remote_copy(
            src_ref=src, dst_ref=dst, send_sem=ssem, recv_sem=rsem,
            device_id=dev, device_id_type=pl.DeviceIdType.MESH,
        )
        copy.start()
        started.append(copy)

    def arrived(dst, ssem, rsem):
        pltpu.make_async_remote_copy(
            src_ref=dst, dst_ref=dst, send_sem=ssem, recv_sem=rsem,
            device_id=sibling, device_id_type=pl.DeviceIdType.MESH,
        ).wait_recv()

    kv_copy = pltpu.make_async_copy(kv_hbm, kv, kv_sem)
    kv_copy.start()
    peers = [sibling]
    peers += [device((x + d) % NX, z, core, y) for d in range(1, NX)]
    peers += [device(x, (z + d) % NZ, core, y) for d in range(1, NZ)]
    peers += [device(x, z, core, (y + d) % NY) for d in range(1, NY)]
    barrier = pltpu.get_barrier_semaphore()
    for peer in peers:
        pl.semaphore_signal(barrier, inc=1, device_id=peer, device_id_type=pl.DeviceIdType.MESH)
    pl.semaphore_wait(barrier, len(peers))

    gathered = (g0, g1)

    def unit_row(key):
        head, xr, zr = key
        xx, zz = along_x(xr), along_z(zr)
        if head == 0:
            return ((core * NZ + zz) * NX + xx) * 2
        return ((core * NX + xx) * NZ + zz) * 2

    count = 0
    done = {}
    own_copies = []
    for key in ARRIVALS:
        head, xr, zr = key
        here = gathered[head].at[pl.ds(unit_row(key), 2)]
        if xr == 0 and zr == 0:
            src = q_ref.at[:, :, pl.ds(head * WIDE, WIDE)]
        else:
            arrived(here, ag_send.at[0], ag_recv.at[UNIT[key]])
            src = here
        for move in onward(key):
            dx, dz = MOVES[move]
            there = UNIT[(head, xr + dx, zr + dz)]
            send(src, here, ag_send.at[count], ag_recv.at[there], link[move])
            count += 1
        if xr == 0 and zr == 0:
            for c in range(2):
                gathered[head][unit_row(key) + c] = q_ref[c, :, head * WIDE : (head + 1) * WIDE]
        bundle = (head, zr if head == 0 else xr)
        done[bundle] = done.get(bundle, 0) + 1
        if head == 0 and done[bundle] == NX:
            zz = along_z(zr)
            rows = g0.at[pl.ds((core * NZ + zz) * NX * 2, NX * 2)]
            send(rows, rows, sg_send.at[zz], sg_recv.at[zz], sibling)
        if head == 1 and done[bundle] == NZ:
            xx = along_x(xr)
            rows = g1.at[pl.ds((core * NX + xx) * NZ * 2, NZ * 2)]
            send(rows, rows, sg_send.at[NZ + xx], sg_recv.at[NZ + xx], sibling)
    for zz in range(NZ):
        rows = g0.at[pl.ds((other * NZ + zz) * NX * 2, NX * 2)]
        arrived(rows, sg_send.at[zz], sg_recv.at[zz])
    for xx in range(NX):
        rows = g1.at[pl.ds((other * NX + xx) * NZ * 2, NZ * 2)]
        arrived(rows, sg_send.at[NZ + xx], sg_recv.at[NZ + xx])
    kv_copy.wait()

    lanes = lax.broadcasted_iota(jnp.int32, (ROWS, 128), 1)

    def query_rows(tile):
        return jnp.concatenate([tile[:, g * 128 : (g + 1) * 128] for g in range(GROUP)], axis=0)

    def score_block(b, carry):
        out = []
        for h in range(2):
            q = query_rows(gathered[h][idx_s[h, b]])
            k = kv[b, 0, :, h * 128 : (h + 1) * 128]
            sc = lax.dot_general(q, k, (((1,), (1,)), ((), ())), preferred_element_type=F32) * SCALE
            sbuf[b, h] = sc
            out.append(jnp.where(lanes == b, jnp.max(sc, axis=1, keepdims=True), carry[h]))
        return tuple(out)

    UNROLL = 4

    def score_step(i, carry):
        for u in range(UNROLL):
            carry = score_block(i * UNROLL + u, carry)
        return carry

    tops = lax.fori_loop(0, SLOTS // UNROLL, score_step, (jnp.full((ROWS, 128), big_neg, F32),) * 2)

    square = lax.broadcasted_iota(jnp.int32, (128, 128), 0)

    def pick(mat, row):
        hot = (square == idx_v[row : row + 1, :]).astype(F32)
        return jnp.dot(mat, hot, precision=lax.Precision.HIGHEST, preferred_element_type=F32)

    tops = tuple(jnp.maximum(t, pick(t, 6)) for t in tops)

    def weigh_block(b, carry):
        out = []
        for h in range(2):
            top = jnp.sum(jnp.where(lanes == b, tops[h], 0.0), axis=1, keepdims=True)
            wt = jnp.exp(sbuf[b, h] - top)
            out.append(jnp.where(lanes == b, jnp.sum(wt, axis=1, keepdims=True), carry[h]))
            v = kv[b, 1, :, h * 128 : (h + 1) * 128]
            res[b, h] = jnp.dot(wt.astype(BF16), v, preferred_element_type=F32)
        return tuple(out)

    def weigh_step(i, carry):
        for u in range(UNROLL):
            carry = weigh_block(i * UNROLL + u, carry)
        return carry

    sums = lax.fori_loop(0, SLOTS // UNROLL, weigh_step, (jnp.zeros((ROWS, 128), F32),) * 2)

    def as_rows(mat):
        return jnp.concatenate([mat, jnp.zeros((128 - ROWS, 128), F32)], axis=0).T

    for h in range(2):
        res[EMPTY, h] = jnp.zeros((ROWS, 128), F32)
        dm[h] = as_rows(pick(tops[h], 2 + 2 * h)).reshape(16, 8, 128)
        dl[h] = as_rows(pick(sums[h], 2 + 2 * h) + pick(sums[h], 3 + 2 * h)).reshape(16, 8, 128)

    def merge(n, sources, emit, normal=False):
        top = sources[0][1]
        for _, m, _ in sources[1:]:
            top = jnp.maximum(top, m)
        total = None
        for i, (_, m, l) in enumerate(sources):
            f = jnp.exp(m - top)
            fscr[i * n : (i + 1) * n, :] = f
            total = l * f if total is None else total + l * f
        width = len(sources) * n
        if normal:
            fscr[width : width + n, :] = 1.0 / total
            width += n
        width = (width + 7) // 8 * 8
        cols = fscr[0:width, :].T
        for j in range(n):
            acc = None
            for i, (load, _, _) in enumerate(sources):
                term = load(j) * cols[:ROWS, i * n + j : i * n + j + 1]
                acc = term if acc is None else acc + term
            if normal:
                at = len(sources) * n + j
                acc = acc * cols[:ROWS, at : at + 1]
            emit(j, acc)
        return top, total

    def held(h, cc, g):
        group = cc * 8 + g

        def load(j):
            at = group * 8 + j
            return res[idx_s[2 + 2 * h, at], h] + res[idx_s[3 + 2 * h, at], h]

        return load, dm[h, group], dl[h, group]

    def group_at(h, k, half):
        return along_z(k) if h == 0 else along_x(k) * 2 + half

    order = []
    for k in (4, 3, -3, 2, -2, 1, -1, 0):
        order.append((0, k, 0))
        if k in (4, 3):
            order += [(1, 2, 0), (1, 2, 1)] if k == 4 else [(1, 1, 0), (1, 1, 1)]
        if k == -3:
            order += [(1, -1, 0), (1, -1, 1)]
        if k == 2:
            order += [(1, 0, 0), (1, 0, 1)]
    for h, k, half in order:
        g = group_at(h, k, half)
        load, m, l = held(h, other, g)
        at = h * 8 + g
        for j in range(8):
            sib_s[at, j] = load(j).astype(BF16)
        sib_ss[at, 0:8, :] = m
        sib_ss[at, 8:16, :] = l
        send(sib_ss.at[at], sib_rs.at[at], sib_send.at[16 + at], sib_recv.at[16 + at], sibling)
        send(sib_s.at[at], sib_r.at[at], sib_send.at[at], sib_recv.at[at], sibling)

    keys = lax.broadcasted_iota(jnp.int32, (ROWS, SPAN), 1)
    tokens = lax.broadcasted_iota(jnp.int32, (ROWS, SPAN), 0) % SPAN
    for h in range(2):
        stat = jnp.zeros((ROWS, 128), F32)
        for c in range(2):
            q = query_rows(q_ref[c, :, h * WIDE : (h + 1) * WIDE])
            k = span_ref[c, 0, :, h * 128 : (h + 1) * 128]
            v = span_ref[c, 1, :, h * 128 : (h + 1) * 128]
            sc = lax.dot_general(q, k, (((1,), (1,)), ((), ())), preferred_element_type=F32) * SCALE
            sc = jnp.where(tokens >= keys, sc, big_neg)
            top = jnp.max(sc, axis=1, keepdims=True)
            wt = jnp.exp(sc - top)
            stat = jnp.where(lanes == c, top, stat)
            stat = jnp.where(lanes == 2 + c, jnp.sum(wt, axis=1, keepdims=True), stat)
            res[OWN + c, h] = jnp.dot(wt.astype(BF16), v, preferred_element_type=F32)
        spst[h] = as_rows(stat)[0:8, :]

    seen = set()

    def from_sibling(h, g):
        at = h * 8 + g
        arrived(sib_rs.at[at], sib_send.at[16 + at], sib_recv.at[16 + at])
        arrived(sib_r.at[at], sib_send.at[at], sib_recv.at[at])
        return (lambda j: sib_r[at, j].astype(F32)), sib_rs[at, 0:8, :], sib_rs[at, 8:16, :]

    def from_ring1(key):
        at = MSG1[key]
        arrived(m1_rs.at[at], m1_send.at[at, 1], m1_recv.at[at, 1])
        arrived(m1_r.at[at], m1_send.at[at, 0], m1_recv.at[at, 0])
        return (lambda j: m1_r[at, j].astype(F32)), m1_rs[at, 0:8, :], m1_rs[at, 8:16, :]

    def from_ring2(key):
        at = MSG2[key]
        arrived(m2_rs.at[at], m2_send.at[at, 1], m2_recv.at[at, 1])
        arrived(m2_r.at[at], m2_send.at[at, 0], m2_recv.at[at, 0])
        return (lambda j: m2_r[at, j].astype(F32)), m2_rs[at, 0:2, :], m2_rs[at, 2:4, :]

    def ring1(h, arm, k, half):
        at = MSG1[(h, arm, k, half)]
        sign = 1 if arm == "L" else -1
        g = group_at(h, sign * k, half)
        sources = [held(h, core, g), from_sibling(h, g)]
        if (h, arm, k + 1, half) in MSG1:
            sources.append(from_ring1((h, arm, k + 1, half)))

        def emit(j, acc):
            m1_s[at, j] = acc.astype(BF16)

        m, l = merge(8, sources, emit)
        m1_ss[at, 0:8, :] = m
        m1_ss[at, 8:16, :] = l
        dev = link[("z" if h == 0 else "x") + ("+" if arm == "L" else "-")]
        send(m1_ss.at[at], m1_rs.at[at], m1_send.at[at, 1], m1_recv.at[at, 1], dev)
        send(m1_s.at[at], m1_r.at[at], m1_send.at[at, 0], m1_recv.at[at, 0], dev)

    def home1(h, half):
        g = group_at(h, 0, half)
        sources = [held(h, core, g), from_sibling(h, g)]
        sources += [from_ring1((h, "L", 1, half)), from_ring1((h, "S", 1, half))]
        acc_ref, stat_ref = (r0, r0s) if h == 0 else (r1, r1s)

        def emit(j, acc):
            acc_ref[half * 8 + j] = acc

        m, l = merge(8, sources, emit)
        for i in range(4):
            stat_ref[half * 4 + i, 0:2, :] = m[2 * i : 2 * i + 2, :]
            stat_ref[half * 4 + i, 2:4, :] = l[2 * i : 2 * i + 2, :]
            stat_ref[half * 4 + i, 4:8, :] = jnp.zeros((4, 128), F32)

    def reduced(h, pos):
        acc_ref, stat_ref = (r0, r0s) if h == 0 else (r1, r1s)
        return (lambda j: acc_ref[pos * 2 + j]), stat_ref[pos, 0:2, :], stat_ref[pos, 2:4, :]

    def ring2(h, arm, k):
        at = MSG2[(h, arm, k)]
        sign = 1 if arm == "L" else -1
        pos = along_x(sign * k) if h == 0 else along_z(sign * k)
        source = reduced(h, pos)
        m2_ss[at, 4:8, :] = jnp.zeros((4, 128), F32)
        if (h, arm, k + 1) in MSG2:

            def emit(j, acc):
                m2_s[at, j] = acc.astype(BF16)

            m, l = merge(2, [source, from_ring2((h, arm, k + 1))], emit)
        else:
            for j in range(2):
                m2_s[at, j] = source[0](j).astype(BF16)
            m, l = source[1], source[2]
        m2_ss[at, 0:2, :] = m
        m2_ss[at, 2:4, :] = l
        dev = link[("x" if h == 0 else "z") + ("+" if arm == "L" else "-")]
        send(m2_ss.at[at], m2_rs.at[at], m2_send.at[at, 1], m2_recv.at[at, 1], dev)
        send(m2_s.at[at], m2_r.at[at], m2_send.at[at, 0], m2_recv.at[at, 0], dev)

    def home2(h):
        span = (lambda j: res[OWN + j, h]), spst[h, 0:2, :], spst[h, 2:4, :]
        pos = x if h == 0 else z
        sources = [reduced(h, pos), from_ring2((h, "L", 1)), from_ring2((h, "S", 1)), span]

        def emit(j, acc):
            for g in range(GROUP):
                col = h * WIDE + g * 128
                att_ref[j, :, col : col + 128] = acc[g * SPAN : (g + 1) * SPAN, :].astype(BF16)

        merge(2, sources, emit, normal=True)

    ring1(0, "L", 4, 0)
    ring1(1, "L", 2, 0)
    ring1(1, "L", 2, 1)
    ring1(0, "S", 3, 0)
    ring1(1, "S", 1, 0)
    ring1(1, "S", 1, 1)
    ring1(0, "L", 3, 0)
    ring1(1, "L", 1, 0)
    ring1(1, "L", 1, 1)
    ring1(0, "S", 2, 0)
    ring1(0, "L", 2, 0)
    home1(1, 0)
    home1(1, 1)
    ring2(1, "L", 4)
    ring2(1, "S", 3)
    ring1(0, "S", 1, 0)
    ring2(1, "L", 3)
    ring2(1, "S", 2)
    ring1(0, "L", 1, 0)
    ring2(1, "L", 2)
    ring2(1, "S", 1)
    home1(0, 0)
    ring2(0, "L", 2)
    ring2(0, "S", 1)
    ring2(1, "L", 1)
    ring2(0, "L", 1)
    home2(1)
    home2(0)

    def bits(ref, src_at, dst_at, sem, dev):
        send(ref.at[src_at], ref.at[dst_at], tail_send.at[sem], tail_recv.at[sem], dev)

    for c in range(2):
        lg[y, c * SPAN : (c + 1) * SPAN, :] = jnp.dot(
            att_ref[c], w_ref[...], preferred_element_type=F32
        )
    for d in range(1, NY):
        bits(lg, y, y, d - 1, device(x, z, core, (y + d) % NY))
    for d in range(1, NY):
        arrived(lg.at[(y + NY - d) % NY], tail_send.at[d - 1], tail_recv.at[d - 1])
    logits = lg[0] + lg[1] + lg[2] + lg[3]
    peak = jnp.max(logits, axis=1, keepdims=True)
    norm = peak + jnp.log(jnp.sum(jnp.exp(logits - peak), axis=1, keepdims=True))
    cand = lax.broadcasted_iota(jnp.int32, (SPAN, NCAND), 1)
    prompt_row = lax.broadcasted_iota(jnp.int32, (8, NCAND), 0)
    cand8 = lax.broadcasted_iota(jnp.int32, (8, NCAND), 1)
    tally = jnp.zeros((8, NCAND), F32)
    for c in range(2):
        rows = slice(c * SPAN, (c + 1) * SPAN)
        chosen = jnp.sum(jnp.where(cand == ans_s[c], logits[rows], 0.0), axis=1, keepdims=True)
        score = jnp.sum(chosen - norm[rows]) * (1.0 / SPAN)
        score_ref[c] = score
        prompt = (dp * 2 + c) // SAMPLES
        tally = tally + jnp.where((prompt_row == prompt) & (cand8 == ans_s[c]), score, 0.0)
    tc[core] = tally
    bits(tc, core, core, 3, sibling)
    arrived(tc.at[other], tail_send.at[3], tail_recv.at[3])
    tx[x] = tc[0] + tc[1]
    for d in range(1, NX):
        bits(tx, x, x, 3 + d, device((x + d) % NX, z, core, y))
    for d in range(1, NX):
        arrived(tx.at[(x + NX - d) % NX], tail_send.at[3 + d], tail_recv.at[3 + d])
    tz[z] = tx[0] + tx[1] + tx[2] + tx[3]
    for d in range(1, NZ):
        bits(tz, z, z, 6 + d, device(x, (z + d) % NZ, core, y))
    for d in range(1, NZ):
        arrived(tz.at[(z + NZ - d) % NZ], tail_send.at[6 + d], tail_recv.at[6 + d])
    whole = tz[0]
    for i in range(1, NZ):
        whole = whole + tz[i]
    for j in range(2):
        tally_ref[:, j : j + 1] = jnp.sum(
            jnp.where(cand8 == dp * 2 + j, whole, 0.0), axis=1, keepdims=True
        )
    for copy in started:
        copy.wait_send()


def tables(tags):
    e = jnp.arange(128, dtype=jnp.int32)
    c = e % 2
    core = e // 64
    chain0 = ((((e // 2) % NX) * NZ + (e // 8) % NZ) * 2 + core) * 2 + c
    chain1 = ((((e // 16) % NX) * NZ + (e // 2) % NZ) * 2 + core) * 2 + c
    padded = jnp.pad(tags, (0, 128 - SLOTS), constant_values=-1)
    tc, tcore, tz, tx = padded % 2, (padded // 2) % 2, (padded // 4) % NZ, padded // (4 * NZ)
    e0 = ((tcore * NZ + tz) * NX + tx) * 2 + tc
    e1 = ((tcore * NX + tx) * NZ + tz) * 2 + tc
    block = jnp.arange(128, dtype=jnp.int32)[None, :]

    def two(chain):
        hit = padded[None, :] == chain[:, None]
        first = jnp.min(jnp.where(hit, block, EMPTY), axis=1)
        second = jnp.max(jnp.where(hit, block, -1), axis=1)
        return first, jnp.where(second > first, second, EMPTY)

    f0, s0 = two(chain0)
    f1, s1 = two(chain1)
    twin = (padded[None, :] == padded[:, None]) & (block != e[:, None]) & (block < SLOTS)
    partner = jnp.max(jnp.where(twin, block, -1), axis=1)
    partner = jnp.where((partner < 0) | (e >= SLOTS), e, partner)
    return jnp.stack([e0, e1, f0, s0, f1, s1, partner, e])


def per_device(queries, key_value_cache, slot_tags, span_key_value, answer_id, w_cand):
    idx = tables(slot_tags)
    vmem = pl.BlockSpec(memory_space=pltpu.VMEM)
    smem = pl.BlockSpec(memory_space=pltpu.SMEM)
    unit = (8, ROWS, 128)
    stat = (16, 128)
    dma = pltpu.SemaphoreType.DMA
    n1, n2 = len(STAGE1), len(STAGE2)
    sends = sum(len(onward(key)) for key in ARRIVALS)
    return pl.pallas_call(
        kernel,
        out_shape=(
            jax.ShapeDtypeStruct((2, SPAN, 2 * WIDE), BF16),
            jax.ShapeDtypeStruct((2,), F32),
            jax.ShapeDtypeStruct((8, 2), F32),
        ),
        in_specs=[vmem, smem, vmem, smem, pl.BlockSpec(memory_space=pl.ANY), vmem, vmem],
        out_specs=(vmem, smem, vmem),
        scratch_shapes=[
            pltpu.VMEM((128, SPAN, WIDE), BF16),
            pltpu.VMEM((128, SPAN, WIDE), BF16),
            pltpu.VMEM(key_value_cache.shape, BF16),
            pltpu.VMEM((SLOTS, 2, ROWS, 128), F32),
            pltpu.VMEM((SLOTS + 3, 2, ROWS, 128), F32),
            pltpu.VMEM((2, 16, 8, 128), F32),
            pltpu.VMEM((2, 16, 8, 128), F32),
            pltpu.VMEM((2, 8, 128), F32),
            pltpu.VMEM((128, 128), F32),
            pltpu.VMEM((16, *unit), BF16),
            pltpu.VMEM((16, *stat), F32),
            pltpu.VMEM((16, *unit), BF16),
            pltpu.VMEM((16, *stat), F32),
            pltpu.VMEM((n1, *unit), BF16),
            pltpu.VMEM((n1, *stat), F32),
            pltpu.VMEM((n1, *unit), BF16),
            pltpu.VMEM((n1, *stat), F32),
            pltpu.VMEM((n2, 2, ROWS, 128), BF16),
            pltpu.VMEM((n2, 8, 128), F32),
            pltpu.VMEM((n2, 2, ROWS, 128), BF16),
            pltpu.VMEM((n2, 8, 128), F32),
            pltpu.VMEM((8, ROWS, 128), F32),
            pltpu.VMEM((4, 8, 128), F32),
            pltpu.VMEM((16, ROWS, 128), F32),
            pltpu.VMEM((8, 8, 128), F32),
            pltpu.VMEM((NY, 2 * SPAN, NCAND), F32),
            pltpu.VMEM((2, 8, 128), F32),
            pltpu.VMEM((NX, 8, 128), F32),
            pltpu.VMEM((NZ, 8, 128), F32),
            dma, dma,
            dma((sends,)), dma((len(ARRIVALS),)), dma((NZ + NX,)), dma((NZ + NX,)),
            dma((32,)), dma((32,)), dma((n1, 2)), dma((n1, 2)), dma((n2, 2)), dma((n2, 2)),
            dma((14,)), dma((14,)),
        ],
        compiler_params=pltpu.CompilerParams(
            collective_id=0, has_side_effects=True, vmem_limit_bytes=60 * 1024 * 1024
        ),
        name="score_chains",
    )(queries, idx, idx, answer_id, key_value_cache, span_key_value, w_cand)


def solution(mesh):
    in_specs = (
        P("dp", None, "mp"),
        P("dp", None, None, "mp"),
        P("dp"),
        P("dp", None, None, "mp"),
        P("dp"),
        P("mp", None),
    )
    out_specs = (P("dp", None, "mp"), P("dp"), P(None, "dp"))
    return jax.shard_map(
        per_device, mesh=mesh, in_specs=in_specs, out_specs=out_specs, check_vma=False
    )
```

```python
import jax
import jax.numpy as jnp
from jax import lax
from jax.experimental import pallas as pl
from jax.experimental.pallas import tpu as pltpu
from jax.sharding import PartitionSpec as P

HEAD_SIZE = 128
NCAND = 128
SAMPLES = 16
SPAN = 16
GROUP = 5
ROWS = SPAN * GROUP
WIDE = GROUP * HEAD_SIZE
SLOTS = 48
EMPTY = SLOTS
OWN = SLOTS + 1
NX, NZ, NY = 4, 8, 4
big_neg = -1e30
SCALE = HEAD_SIZE ** (-0.5)
F32 = jnp.float32
BF16 = jnp.bfloat16

ARRIVALS = [
    (0, 0, 0), (1, 0, 0), (0, -1, 0), (0, 0, -1), (0, 0, 1), (0, 1, 0), (1, 0, -1), (1, 0, 1),
    (1, 1, 0), (0, -2, 0), (1, 0, -2), (1, 0, 2), (1, -1, 0), (0, -1, -1), (0, -1, 1), (1, -1, -1),
    (1, 1, -1), (0, 0, -2), (0, 0, 2), (1, -1, 1), (1, 1, 1), (0, 1, -1), (0, 1, 1), (1, -1, -2),
    (1, 1, -2), (1, -1, 2), (1, 1, 2), (1, 0, -3), (1, 0, 3), (1, -2, 0), (0, -2, -1), (0, -2, 1),
    (1, -2, -1), (0, -1, 2), (1, -2, 1), (1, 0, -4), (0, 0, 3), (1, 1, -3), (1, -2, -2), (0, -1, -2),
    (0, 1, 2), (1, 1, 3), (1, -2, 2), (0, -2, 2), (0, 0, -3), (1, -1, -3), (0, -1, 3), (0, 1, -2),
    (1, 1, -4), (1, -1, 3), (0, -2, -2), (1, -1, -4), (0, 1, 3), (0, -1, -3), (0, -2, 3), (0, 0, -4),
    (1, -2, -3), (0, 1, -3), (1, -2, 3), (0, -2, -3), (1, -2, -4), (0, -1, -4), (0, 1, -4), (0, -2, -4),
]
UNIT = {key: i for i, key in enumerate(ARRIVALS)}
MOVES = {
    "x+": (-1, 0), "x-": (1, 0), "z+": (0, -1), "z-": (0, 1),
    "x++": (-2, 0), "z++": (0, -2), "z--": (0, 2),
}


def onward(key):
    head, xr, zr = key
    out = []
    if head == 1:
        if xr == 0:
            if zr == 0:
                out += ["z+", "z-", "z++", "z--"]
            if zr in (-1, -2):
                out.append("z++")
            if zr == 1:
                out.append("z--")
        if -2 < xr <= 0:
            out.append("x+")
        if 0 <= xr < 1:
            out.append("x-")
    else:
        if -4 < zr <= 0:
            out.append("z+")
        if 0 <= zr < 3:
            out.append("z-")
        if xr == 0 and zr == 0:
            out += ["x+", "x-", "x++"]
    return out


STAGE1 = [(0, arm, k, half) for arm, top in (("L", 4), ("S", 3)) for k in range(1, top + 1) for half in (0, 1)]
STAGE1 += [(1, arm, k, half) for arm, top in (("L", 2), ("S", 1)) for k in range(1, top + 1) for half in (0, 1)]
STAGE2 = {
    (0, "L", 2): ("x++", None), (0, "L", 1): ("x+", None), (0, "S", 1): ("x-", None),
    (1, "L", 4): ("z++", None), (1, "L", 3): ("z++", None),
    (1, "S", 3): ("z--", None), (1, "S", 2): ("z--", None),
    (1, "L", 2): ("z++", (1, "L", 4)), (1, "L", 1): ("z+", (1, "L", 3)), (1, "S", 1): ("z-", (1, "S", 3)),
}
LAST = ([("L", 2), ("L", 1), ("S", 1)], [("L", 2), ("L", 1), ("S", 1), ("S", 2)])
MSG1 = {key: i for i, key in enumerate(STAGE1)}
MSG2 = {key: i for i, key in enumerate(STAGE2)}
STEPS = [
    ("sb", 0, 4, 0), ("sb", 1, 2, 0), ("sb", 1, 2, 1), ("sb", 0, -3, 0),
    ("sb", 0, 3, 0), ("sb", 0, -2, 0), ("r1", 0, "L", 4, 0), ("r1", 0, "L", 4, 1),
    ("r1", 1, "L", 2, 0), ("r1", 1, "L", 2, 1), ("sb", 0, 2, 0), ("r1", 0, "S", 3, 0),
    ("r1", 0, "S", 3, 1), ("sb", 1, -1, 0), ("sb", 1, -1, 1), ("sb", 1, 1, 0),
    ("sb", 1, 1, 1), ("sb", 0, -1, 0), ("sb", 0, 1, 0), ("sb", 0, 0, 0),
    ("sb", 1, 0, 0), ("sb", 1, 0, 1), ("r1", 1, "S", 1, 0), ("r1", 1, "S", 1, 1),
    ("r1", 0, "L", 3, 0), ("r1", 0, "S", 2, 0), ("r1", 0, "L", 3, 1), ("r1", 1, "L", 1, 0),
    ("r1", 0, "S", 2, 1), ("r1", 0, "L", 2, 0), ("r1", 0, "S", 1, 0), ("r1", 1, "L", 1, 1),
    ("r1", 0, "L", 2, 1), ("r1", 0, "S", 1, 1), ("r1", 0, "L", 1, 0), ("h1", 1, 0),
    ("r1", 0, "L", 1, 1), ("h1", 1, 1), ("r2", 1, "L", 4), ("r2", 1, "L", 3),
    ("r2", 1, "S", 3), ("r2", 1, "S", 2), ("h1", 0, 0), ("h1", 0, 1),
    ("r2", 0, "L", 2), ("r2", 0, "L", 1), ("r2", 0, "S", 1), ("r2", 1, "L", 2),
    ("r2", 1, "S", 1), ("r2", 1, "L", 1), ("h2", 0), ("h2", 1),
]


def kernel(
    q_hbm, idx_s, idx_v, ans_s, kv_hbm, span_hbm, w_hbm,
    att_ref, small_ref,
    q_ref, span_ref, w_ref, ring_tally,
    g0, g1, kv, sbuf, res, dm, dl, spst, fscr,
    sib_s, sib_ss, sib_r, sib_rs, m1_s, m1_ss, m1_r, m1_rs, m2_s, m2_ss, m2_r, m2_rs,
    r0, r0s, r1, r1s, lg, ta, tz,
    in_sem, ag_send, ag_recv, sg_send, sg_recv,
    sib_send, sib_recv, m1_send, m1_recv, m2_send, m2_recv, tail_send, tail_recv,
):
    dp = lax.axis_index("dp")
    y = lax.axis_index("mp")
    core = dp % 2
    z = (dp // 2) % NZ
    x = dp // (2 * NZ)
    s = 1 - 2 * core
    other = 1 - core

    def device(xx, zz, cc, yy):
        return (xx * (2 * NZ) + zz * 2 + cc, yy)

    def along_x(k):
        return (x + s * k + 2 * NX) % NX

    def along_z(k):
        return (z + s * k + 2 * NZ) % NZ

    sibling = device(x, z, other, y)
    link = {
        "x+": device(along_x(1), z, core, y),
        "x-": device(along_x(-1), z, core, y),
        "z+": device(x, along_z(1), core, y),
        "z-": device(x, along_z(-1), core, y),
        "x++": device(along_x(2), z, core, y),
        "z++": device(x, along_z(2), core, y),
        "z--": device(x, along_z(-2), core, y),
    }
    started = []

    def send(src, dst, ssem, rsem, dev):
        copy = pltpu.make_async_remote_copy(
            src_ref=src, dst_ref=dst, send_sem=ssem, recv_sem=rsem,
            device_id=dev, device_id_type=pl.DeviceIdType.MESH,
        )
        copy.start()
        started.append(copy)

    def arrived(dst, ssem, rsem):
        pltpu.make_async_remote_copy(
            src_ref=dst, dst_ref=dst, send_sem=ssem, recv_sem=rsem,
            device_id=sibling, device_id_type=pl.DeviceIdType.MESH,
        ).wait_recv()

    q_copy = pltpu.make_async_copy(q_hbm, q_ref, in_sem.at[0])
    kv_copy = pltpu.make_async_copy(kv_hbm, kv, in_sem.at[1])
    span_copy = pltpu.make_async_copy(span_hbm, span_ref, in_sem.at[2])
    w_copy = pltpu.make_async_copy(w_hbm, w_ref, in_sem.at[3])
    q_copy.start()
    peers = [sibling]
    peers += [device((x + d) % NX, z, core, y) for d in range(1, NX)]
    peers += [device(x, (z + d) % NZ, core, y) for d in (1, 2, NZ - 2, NZ - 1)]
    peers += [device(x, z, core, (y + d) % NY) for d in range(1, NY)]
    barrier = pltpu.get_barrier_semaphore()
    for peer in peers:
        pl.semaphore_signal(barrier, inc=1, device_id=peer, device_id_type=pl.DeviceIdType.MESH)
    span_copy.start()
    w_copy.start()
    q_copy.wait()
    pl.semaphore_wait(barrier, len(peers))

    gathered = (g0, g1)

    def unit_row(key):
        head, xr, zr = key
        xx, zz = along_x(xr), along_z(zr)
        if head == 0:
            return ((core * NZ + zz) * NX + xx) * 2
        return ((core * NX + xx) * NZ + zz) * 2

    lanes = lax.broadcasted_iota(jnp.int32, (ROWS, 128), 1)

    def query_rows(tile):
        return jnp.concatenate([tile[:, g * 128 : (g + 1) * 128] for g in range(GROUP)], axis=0)

    def as_rows(mat):
        return jnp.concatenate([mat, jnp.zeros((128 - ROWS, 128), F32)], axis=0).T

    def own_spans():
        span_copy.wait()
        keys = lax.broadcasted_iota(jnp.int32, (ROWS, SPAN), 1)
        tokens = lax.broadcasted_iota(jnp.int32, (ROWS, SPAN), 0) % SPAN
        for h in range(2):
            stat = jnp.zeros((ROWS, 128), F32)
            for c in range(2):
                q = query_rows(q_ref[c, :, h * WIDE : (h + 1) * WIDE])
                k = span_ref[c, 0, :, h * 128 : (h + 1) * 128]
                v = span_ref[c, 1, :, h * 128 : (h + 1) * 128]
                sc = lax.dot_general(q, k, (((1,), (1,)), ((), ())), preferred_element_type=F32) * SCALE
                sc = jnp.where(tokens >= keys, sc, big_neg)
                top = jnp.max(sc, axis=1, keepdims=True)
                wt = jnp.exp(sc - top)
                stat = jnp.where(lanes == c, top, stat)
                stat = jnp.where(lanes == 2 + c, jnp.sum(wt, axis=1, keepdims=True), stat)
                res[OWN + c, h] = jnp.dot(wt.astype(BF16), v, preferred_element_type=F32)
            spst[h] = as_rows(stat)[0:8, :]

    count = 0
    done = {}
    for step, key in enumerate(ARRIVALS):
        if step == 2:
            kv_copy.start()
        if step == 12:
            own_spans()
        head, xr, zr = key
        here = gathered[head].at[pl.ds(unit_row(key), 2)]
        if xr == 0 and zr == 0:
            src = q_ref.at[:, :, pl.ds(head * WIDE, WIDE)]
        else:
            arrived(here, ag_send.at[0], ag_recv.at[UNIT[key]])
            src = here
        for move in onward(key):
            dx, dz = MOVES[move]
            there = UNIT[(head, xr + dx, zr + dz)]
            send(src, here, ag_send.at[count], ag_recv.at[there], link[move])
            count += 1
        if xr == 0 and zr == 0:
            for c in range(2):
                gathered[head][unit_row(key) + c] = q_ref[c, :, head * WIDE : (head + 1) * WIDE]
        bundle = (head, zr if head == 0 else xr)
        done[bundle] = done.get(bundle, 0) + 1
        if head == 0 and done[bundle] == NX:
            zz = along_z(zr)
            rows = g0.at[pl.ds((core * NZ + zz) * NX * 2, NX * 2)]
            send(rows, rows, sg_send.at[zz], sg_recv.at[zz], sibling)
        if head == 1 and done[bundle] == NZ:
            xx = along_x(xr)
            rows = g1.at[pl.ds((core * NX + xx) * NZ * 2, NZ * 2)]
            send(rows, rows, sg_send.at[NZ + xx], sg_recv.at[NZ + xx], sibling)
    for zz in range(NZ):
        rows = g0.at[pl.ds((other * NZ + zz) * NX * 2, NX * 2)]
        arrived(rows, sg_send.at[zz], sg_recv.at[zz])
    for xx in range(NX):
        rows = g1.at[pl.ds((other * NX + xx) * NZ * 2, NZ * 2)]
        arrived(rows, sg_send.at[NZ + xx], sg_recv.at[NZ + xx])
    kv_copy.wait()

    def score_block(b, carry):
        out = []
        for h in range(2):
            q = query_rows(gathered[h][idx_s[h, b]])
            k = kv[b, 0, :, h * 128 : (h + 1) * 128]
            sc = lax.dot_general(q, k, (((1,), (1,)), ((), ())), preferred_element_type=F32) * SCALE
            sbuf[b, h] = sc
            out.append(jnp.where(lanes == b, jnp.max(sc, axis=1, keepdims=True), carry[h]))
        return tuple(out)

    UNROLL = 4

    def score_step(i, carry):
        for u in range(UNROLL):
            carry = score_block(i * UNROLL + u, carry)
        return carry

    tops = lax.fori_loop(0, SLOTS // UNROLL, score_step, (jnp.full((ROWS, 128), big_neg, F32),) * 2)

    square = lax.broadcasted_iota(jnp.int32, (128, 128), 0)

    def pick(mat, wanted):
        hot = (square == wanted).astype(F32)
        return jnp.dot(mat, hot, precision=lax.Precision.HIGHEST, preferred_element_type=F32)

    twin = idx_v[6:7, :]
    twin = jnp.where(twin < 0, lax.broadcasted_iota(jnp.int32, (1, 128), 1), twin)
    tops = tuple(jnp.maximum(t, pick(t, twin)) for t in tops)

    def weigh_block(b, carry):
        out = []
        for h in range(2):
            top = jnp.sum(jnp.where(lanes == b, tops[h], 0.0), axis=1, keepdims=True)
            wt = jnp.exp(sbuf[b, h] - top)
            out.append(jnp.where(lanes == b, jnp.sum(wt, axis=1, keepdims=True), carry[h]))
            v = kv[b, 1, :, h * 128 : (h + 1) * 128]
            res[b, h] = jnp.dot(wt.astype(BF16), v, preferred_element_type=F32)
        return tuple(out)

    def weigh_step(i, carry):
        for u in range(UNROLL):
            carry = weigh_block(i * UNROLL + u, carry)
        return carry

    sums = lax.fori_loop(0, SLOTS // UNROLL, weigh_step, (jnp.zeros((ROWS, 128), F32),) * 2)

    for h in range(2):
        res[EMPTY, h] = jnp.zeros((ROWS, 128), F32)
        first = EMPTY - idx_v[2 + 2 * h : 3 + 2 * h, :]
        last = idx_v[3 + 2 * h : 4 + 2 * h, :]
        last = jnp.where(last > first, last, EMPTY)
        dm[h] = as_rows(pick(tops[h], first)).reshape(16, 8, 128)
        dl[h] = as_rows(pick(sums[h], first) + pick(sums[h], last)).reshape(16, 8, 128)

    def merge(n, sources, emit, normal=False):
        top = sources[0][1]
        for _, m, _ in sources[1:]:
            top = jnp.maximum(top, m)
        total = None
        for i, (_, m, l) in enumerate(sources):
            f = jnp.exp(m - top)
            fscr[i * n : (i + 1) * n, :] = f
            total = l * f if total is None else total + l * f
        width = len(sources) * n
        if normal:
            fscr[width : width + n, :] = 1.0 / total
            width += n
        width = (width + 7) // 8 * 8
        cols = fscr[0:width, :].T
        for j in range(n):
            acc = None
            for i, (load, _, _) in enumerate(sources):
                term = load(j) * cols[:ROWS, i * n + j : i * n + j + 1]
                acc = term if acc is None else acc + term
            if normal:
                at = len(sources) * n + j
                acc = acc * cols[:ROWS, at : at + 1]
            emit(j, acc)
        return top, total

    def held(h, cc, g, first, n):
        group = cc * 8 + g

        def load(j):
            at = group * 8 + first + j
            one, two = EMPTY - idx_s[2 + 2 * h, at], idx_s[3 + 2 * h, at]
            return res[one, h] + res[jnp.where(two > one, two, EMPTY), h]

        return load, dm[h, group, first : first + n, :], dl[h, group, first : first + n, :]

    def group_at(h, k, half):
        return along_z(k) if h == 0 else along_x(k) * 2 + half

    def to_sibling(h, k, half):
        g = group_at(h, k, half)
        load, m, l = held(h, other, g, 0, 8)
        at = h * 8 + g
        for j in range(8):
            sib_s[at, j] = load(j).astype(BF16)
        sib_ss[at, 0:8, :] = m
        sib_ss[at, 8:16, :] = l
        send(sib_ss.at[at], sib_rs.at[at], sib_send.at[16 + at], sib_recv.at[16 + at], sibling)
        send(sib_s.at[at], sib_r.at[at], sib_send.at[at], sib_recv.at[at], sibling)

    seen = set()

    def from_sibling(h, g, key, first, n):
        at = h * 8 + g
        if key not in seen:
            seen.add(key)
            arrived(sib_rs.at[at], sib_send.at[16 + at], sib_recv.at[16 + at])
            arrived(sib_r.at[at], sib_send.at[at], sib_recv.at[at])
        stat = sib_rs[at, first : first + n, :], sib_rs[at, 8 + first : 8 + first + n, :]
        return (lambda j: sib_r[at, first + j].astype(F32)), *stat

    def from_ring1(key, n):
        at = MSG1[key]
        arrived(m1_rs.at[at, pl.ds(0, 2 * n)], m1_send.at[at, 1], m1_recv.at[at, 1])
        arrived(m1_r.at[at, pl.ds(0, n)], m1_send.at[at, 0], m1_recv.at[at, 0])
        return (lambda j: m1_r[at, j].astype(F32)), m1_rs[at, 0:n, :], m1_rs[at, n : 2 * n, :]

    def from_ring2(key):
        at = MSG2[key]
        arrived(m2_rs.at[at], m2_send.at[at, 1], m2_recv.at[at, 1])
        arrived(m2_r.at[at], m2_send.at[at, 0], m2_recv.at[at, 0])
        return (lambda j: m2_r[at, j].astype(F32)), m2_rs[at, 0:2, :], m2_rs[at, 2:4, :]

    def local(h, k, half):
        g = group_at(h, k, half)
        first, n = (half * 4, 4) if h == 0 else (0, 8)
        key = (h, k) if h == 0 else (h, k, half)
        return n, [held(h, core, g, first, n), from_sibling(h, g, key, first, n)]

    def ring1(h, arm, k, half):
        at = MSG1[(h, arm, k, half)]
        n, sources = local(h, k if arm == "L" else -k, half)
        if (h, arm, k + 1, half) in MSG1:
            sources.append(from_ring1((h, arm, k + 1, half), n))

        def emit(j, acc):
            m1_s[at, j] = acc.astype(BF16)

        m, l = merge(n, sources, emit)
        m1_ss[at, 0:n, :] = m
        m1_ss[at, n : 2 * n, :] = l
        dev = link[("z" if h == 0 else "x") + ("+" if arm == "L" else "-")]
        stat, data = pl.ds(0, 2 * n), pl.ds(0, n)
        send(m1_ss.at[at, stat], m1_rs.at[at, stat], m1_send.at[at, 1], m1_recv.at[at, 1], dev)
        send(m1_s.at[at, data], m1_r.at[at, data], m1_send.at[at, 0], m1_recv.at[at, 0], dev)

    def home1(h, half):
        n, sources = local(h, 0, half)
        sources += [from_ring1((h, "L", 1, half), n), from_ring1((h, "S", 1, half), n)]
        acc_ref, stat_ref = (r0, r0s) if h == 0 else (r1, r1s)

        def emit(j, acc):
            acc_ref[half * n + j] = acc

        m, l = merge(n, sources, emit)
        for i in range(n // 2):
            at = half * (n // 2) + i
            stat_ref[at, 0:2, :] = m[2 * i : 2 * i + 2, :]
            stat_ref[at, 2:4, :] = l[2 * i : 2 * i + 2, :]

    def reduced(h, pos):
        acc_ref, stat_ref = (r0, r0s) if h == 0 else (r1, r1s)
        return (lambda j: acc_ref[pos * 2 + j]), stat_ref[pos, 0:2, :], stat_ref[pos, 2:4, :]

    def ring2(h, arm, k):
        at = MSG2[(h, arm, k)]
        move, joins = STAGE2[(h, arm, k)]
        offset = k if arm == "L" else -k
        source = reduced(h, along_x(offset) if h == 0 else along_z(offset))
        if joins is None:
            for j in range(2):
                m2_s[at, j] = source[0](j).astype(BF16)
            m, l = source[1], source[2]
        else:

            def emit(j, acc):
                m2_s[at, j] = acc.astype(BF16)

            m, l = merge(2, [source, from_ring2(joins)], emit)
        m2_ss[at, 0:2, :] = m
        m2_ss[at, 2:4, :] = l
        m2_ss[at, 4:8, :] = jnp.zeros((4, 128), F32)
        send(m2_ss.at[at], m2_rs.at[at], m2_send.at[at, 1], m2_recv.at[at, 1], link[move])
        send(m2_s.at[at], m2_r.at[at], m2_send.at[at, 0], m2_recv.at[at, 0], link[move])

    def home2(h):
        span = (lambda j: res[OWN + j, h]), spst[h, 0:2, :], spst[h, 2:4, :]
        sources = [reduced(h, x if h == 0 else z), span]
        sources += [from_ring2((h, *last)) for last in LAST[h]]

        def emit(j, acc):
            for g in range(GROUP):
                col = h * WIDE + g * 128
                att_ref[j, :, col : col + 128] = acc[g * SPAN : (g + 1) * SPAN, :].astype(BF16)

        merge(2, sources, emit, normal=True)

    run = {"sb": to_sibling, "r1": ring1, "h1": home1, "r2": ring2, "h2": home2}
    for step in STEPS:
        run[step[0]](*step[1:])

    w_copy.wait()
    def bits(ref, src_at, dst_at, sem, dev):
        send(ref.at[src_at], ref.at[dst_at], tail_send.at[sem], tail_recv.at[sem], dev)

    for c in range(2):
        lg[y, c * SPAN : (c + 1) * SPAN, :] = jnp.dot(
            att_ref[c], w_ref[...], preferred_element_type=F32
        )
    for d in range(1, NY):
        bits(lg, y, y, d - 1, device(x, z, core, (y + d) % NY))
    for d in range(1, NY):
        arrived(lg.at[(y + NY - d) % NY], tail_send.at[d - 1], tail_recv.at[d - 1])
    logits = lg[0] + lg[1] + lg[2] + lg[3]
    peak = jnp.max(logits, axis=1, keepdims=True)
    norm = peak + jnp.log(jnp.sum(jnp.exp(logits - peak), axis=1, keepdims=True))
    cand = lax.broadcasted_iota(jnp.int32, (SPAN, NCAND), 1)
    prompt_row = lax.broadcasted_iota(jnp.int32, (8, NCAND), 0)
    cand8 = lax.broadcasted_iota(jnp.int32, (8, NCAND), 1)
    tally = jnp.zeros((8, NCAND), F32)
    scores = []
    for c in range(2):
        rows = slice(c * SPAN, (c + 1) * SPAN)
        chosen = jnp.sum(jnp.where(cand == ans_s[c], logits[rows], 0.0), axis=1, keepdims=True)
        score = jnp.sum(chosen - norm[rows]) * (1.0 / SPAN)
        scores.append(score)
        prompt = (dp * 2 + c) // SAMPLES
        tally = tally + jnp.where((prompt_row == prompt) & (cand8 == ans_s[c]), score, 0.0)
    here = x * 2 + core
    ta[here] = tally
    for d in range(1, 2 * NX):
        dx, dc = d // 2, d % 2
        dev = device((x + dx) % NX, z, (core + dc) % 2, y)
        bits(ta, here, here, 2 + d, dev)
    for d in range(1, 2 * NX):
        dx, dc = d // 2, d % 2
        source = (x + NX - dx) % NX * 2 + (core + dc) % 2
        arrived(ta.at[source], tail_send.at[2 + d], tail_recv.at[2 + d])
    part = ta[0]
    for i in range(1, 2 * NX):
        part = part + ta[i]
    tz[z] = part
    for d in range(1, NZ):
        bits(tz, z, z, 9 + d, device(x, (z + d) % NZ, core, y))
    for d in range(1, NZ):
        arrived(tz.at[(z + NZ - d) % NZ], tail_send.at[9 + d], tail_recv.at[9 + d])
    whole = tz[0]
    for i in range(1, NZ):
        whole = whole + tz[i]
    ring_tally[:, 0:8] = whole.T
    small_ref[0:2, :] = jnp.zeros((2, 128), F32)
    small_ref[0:2, 0:8] = ring_tally[pl.ds(dp * 2, 2), 0:8]
    row = lax.broadcasted_iota(jnp.int32, (2, 128), 0)
    small_ref[2:4, :] = jnp.where(row == 0, scores[0], scores[1])
    small_ref[4:8, :] = jnp.zeros((4, 128), F32)
    for copy in started:
        copy.wait_send()


def hand_out(att_ref, small_ref, out_ref, score_ref, tally_ref):
    out_ref[...] = att_ref[...]
    tally_ref[...] = small_ref[0:2, 0:8]
    score_ref[0] = small_ref[2, 0]
    score_ref[1] = small_ref[3, 0]


def tables(tags):
    r, e, b = (lax.broadcasted_iota(jnp.int32, (8, 128, 128), axis) for axis in range(3))
    c, core = e % 2, e // 64
    chain0 = ((((e // 2) % NX) * NZ + (e // 8) % NZ) * 2 + core) * 2 + c
    chain1 = ((((e // 16) % NX) * NZ + (e // 2) % NZ) * 2 + core) * 2 + c
    padded = jnp.pad(tags, (0, 128 - SLOTS), constant_values=-1)
    tag, mine = padded[None, None, :], padded[None, :, None]
    tc, tcore, tz, tx = tag % 2, (tag // 2) % 2, (tag // 4) % NZ, tag // (4 * NZ)
    place0 = ((tcore * NZ + tz) * NX + tx) * 2 + tc
    place1 = ((tcore * NX + tx) * NZ + tz) * 2 + tc
    wanted = jnp.where(r < 4, chain0, jnp.where(r < 6, chain1, mine))
    hit = jnp.where(r < 2, b == e, (tag == wanted) & ((r < 6) | (b != e))) & (b < SLOTS)
    first = (r == 2) | (r == 4)
    value = jnp.where(first, EMPTY - b, jnp.where(r == 0, place0, jnp.where(r == 1, place1, b)))
    return jnp.max(jnp.where(hit, value, jnp.where(first, 0, -1)), axis=2)


def per_device(queries, key_value_cache, slot_tags, span_key_value, answer_id, w_cand):
    idx = tables(slot_tags)
    vmem = pl.BlockSpec(memory_space=pltpu.VMEM)
    smem = pl.BlockSpec(memory_space=pltpu.SMEM)
    anywhere = pl.BlockSpec(memory_space=pl.ANY)
    unit = (8, ROWS, 128)
    stat = (16, 128)
    dma = pltpu.SemaphoreType.DMA
    n1, n2 = len(STAGE1), len(STAGE2)
    sends = sum(len(onward(key)) for key in ARRIVALS)
    attended, small = pl.pallas_call(
        kernel,
        out_shape=(
            jax.ShapeDtypeStruct((2, SPAN, 2 * WIDE), BF16),
            jax.ShapeDtypeStruct((8, 128), F32),
        ),
        in_specs=[anywhere, smem, vmem, smem, anywhere, anywhere, anywhere],
        out_specs=(vmem, vmem),
        scratch_shapes=[
            pltpu.VMEM(queries.shape, BF16),
            pltpu.VMEM(span_key_value.shape, BF16),
            pltpu.VMEM(w_cand.shape, BF16),
            pltpu.VMEM((128, 128), F32),
            pltpu.VMEM((128, SPAN, WIDE), BF16),
            pltpu.VMEM((128, SPAN, WIDE), BF16),
            pltpu.VMEM(key_value_cache.shape, BF16),
            pltpu.VMEM((SLOTS, 2, ROWS, 128), F32),
            pltpu.VMEM((SLOTS + 3, 2, ROWS, 128), F32),
            pltpu.VMEM((2, 16, 8, 128), F32),
            pltpu.VMEM((2, 16, 8, 128), F32),
            pltpu.VMEM((2, 8, 128), F32),
            pltpu.VMEM((128, 128), F32),
            pltpu.VMEM((16, *unit), BF16),
            pltpu.VMEM((16, *stat), F32),
            pltpu.VMEM((16, *unit), BF16),
            pltpu.VMEM((16, *stat), F32),
            pltpu.VMEM((n1, *unit), BF16),
            pltpu.VMEM((n1, *stat), F32),
            pltpu.VMEM((n1, *unit), BF16),
            pltpu.VMEM((n1, *stat), F32),
            pltpu.VMEM((n2, 2, ROWS, 128), BF16),
            pltpu.VMEM((n2, 8, 128), F32),
            pltpu.VMEM((n2, 2, ROWS, 128), BF16),
            pltpu.VMEM((n2, 8, 128), F32),
            pltpu.VMEM((8, ROWS, 128), F32),
            pltpu.VMEM((4, 8, 128), F32),
            pltpu.VMEM((16, ROWS, 128), F32),
            pltpu.VMEM((8, 8, 128), F32),
            pltpu.VMEM((NY, 2 * SPAN, NCAND), F32),
            pltpu.VMEM((2 * NX, 8, 128), F32),
            pltpu.VMEM((NZ, 8, 128), F32),
            dma((4,)),
            dma((sends,)), dma((len(ARRIVALS),)), dma((NZ + NX,)), dma((NZ + NX,)),
            dma((32,)), dma((32,)), dma((n1, 2)), dma((n1, 2)), dma((n2, 2)), dma((n2, 2)),
            dma((17,)), dma((17,)),
        ],
        compiler_params=pltpu.CompilerParams(
            collective_id=0, has_side_effects=True, vmem_limit_bytes=60 * 1024 * 1024
        ),
        name="score_chains",
    )(queries, idx, idx, answer_id, key_value_cache, span_key_value, w_cand)
    attended, score, tally = pl.pallas_call(
        hand_out,
        out_shape=(
            jax.ShapeDtypeStruct(attended.shape, BF16),
            jax.ShapeDtypeStruct((2,), F32),
            jax.ShapeDtypeStruct((2, 8), F32),
        ),
        in_specs=[vmem, vmem],
        out_specs=(vmem, smem, vmem),
        name="hand_out",
    )(attended, small)
    return attended, score, tally.T


def solution(mesh):
    in_specs = (
        P("dp", None, "mp"),
        P("dp", None, None, "mp"),
        P("dp"),
        P("dp", None, None, "mp"),
        P("dp"),
        P("mp", None),
    )
    out_specs = (P("dp", None, "mp"), P("dp"), P(None, "dp"))
    return jax.shard_map(
        per_device, mesh=mesh, in_specs=in_specs, out_specs=out_specs, check_vma=False
    )
```

```python
import jax
import jax.numpy as jnp
from jax import lax
from jax.experimental import pallas as pl
from jax.experimental.pallas import tpu as pltpu
from jax.sharding import PartitionSpec as P

HEAD_SIZE = 128
NCAND = 128
SAMPLES = 16
SPAN = 16
GROUP = 5
ROWS = SPAN * GROUP
WIDE = GROUP * HEAD_SIZE
SLOTS = 48
EMPTY = SLOTS
OWN = SLOTS + 1
NX, NZ, NY = 4, 8, 4
UNROLL = 8
big_neg = -1e30
SCALE = HEAD_SIZE ** (-0.5)
F32 = jnp.float32
BF16 = jnp.bfloat16

ARRIVALS = [
    (0, 0, 0), (1, 0, 0), (0, -1, 0), (0, 0, -1), (0, 0, 1), (0, 1, 0), (1, 0, -1), (1, 0, 1),
    (1, 1, 0), (0, -2, 0), (1, 0, -2), (1, 0, 2), (1, -1, 0), (0, -1, -1), (0, -1, 1), (1, -1, -1),
    (1, 1, -1), (0, 0, -2), (0, 0, 2), (1, -1, 1), (1, 1, 1), (0, 1, -1), (0, 1, 1), (1, -1, -2),
    (1, 1, -2), (1, -1, 2), (1, 1, 2), (1, 0, -3), (1, 0, 3), (1, -2, 0), (0, -2, -1), (0, -2, 1),
    (1, -2, -1), (0, -1, 2), (1, -2, 1), (1, 0, -4), (0, 0, 3), (1, 1, -3), (1, -2, -2), (0, -1, -2),
    (0, 1, 2), (1, 1, 3), (1, -2, 2), (0, -2, 2), (0, 0, -3), (1, -1, -3), (0, -1, 3), (0, 1, -2),
    (1, 1, -4), (1, -1, 3), (0, -2, -2), (1, -1, -4), (0, 1, 3), (0, -1, -3), (0, -2, 3), (0, 0, -4),
    (1, -2, -3), (0, 1, -3), (1, -2, 3), (0, -2, -3), (1, -2, -4), (0, -1, -4), (0, 1, -4), (0, -2, -4),
]
UNIT = {key: i for i, key in enumerate(ARRIVALS)}
MOVES = {
    "x+": (-1, 0), "x-": (1, 0), "z+": (0, -1), "z-": (0, 1),
    "x++": (-2, 0), "z++": (0, -2), "z--": (0, 2),
}


def onward(key):
    head, xr, zr = key
    out = []
    if head == 1:
        if xr == 0:
            if zr == 0:
                out += ["z+", "z-", "z++", "z--"]
            if zr in (-1, -2):
                out.append("z++")
            if zr == 1:
                out.append("z--")
        if -2 < xr <= 0:
            out.append("x+")
        if 0 <= xr < 1:
            out.append("x-")
    else:
        if -4 < zr <= 0:
            out.append("z+")
        if 0 <= zr < 3:
            out.append("z-")
        if xr == 0 and zr == 0:
            out += ["x+", "x-", "x++"]
    return out


STAGE1 = [(0, arm, k, half) for arm, top in (("L", 4), ("S", 3)) for k in range(1, top + 1) for half in (0, 1)]
STAGE1 += [(1, arm, k, part) for arm, top in (("L", 2), ("S", 1)) for k in range(1, top + 1) for part in range(4)]
STAGE2 = {
    (0, "L", 2): ("x++", None), (0, "L", 1): ("x+", None), (0, "S", 1): ("x-", None),
    (1, "L", 4): ("z++", None), (1, "L", 3): ("z++", None),
    (1, "S", 3): ("z--", None), (1, "S", 2): ("z--", None),
    (1, "L", 2): ("z++", (1, "L", 4)), (1, "L", 1): ("z+", (1, "L", 3)), (1, "S", 1): ("z-", (1, "S", 3)),
}
LAST = ([("L", 2), ("L", 1), ("S", 1)], [("L", 2), ("L", 1), ("S", 1), ("S", 2)])
MSG1 = {key: i for i, key in enumerate(STAGE1)}
MSG2 = {key: i for i, key in enumerate(STAGE2)}
STEPS = [
    ("sb", 0, 4, 0), ("sb", 1, 2, 0), ("sb", 1, 2, 1), ("sb", 0, -3, 0),
    ("sb", 0, 3, 0), ("sb", 0, -2, 0), ("sb", 0, 2, 0), ("sb", 1, -1, 0),
    ("sb", 1, -1, 1), ("sb", 1, 1, 0), ("sb", 1, 1, 1), ("r1", 0, "L", 4, 0),
    ("r1", 0, "L", 4, 1), ("r1", 1, "L", 2, 0), ("r1", 1, "L", 2, 1), ("r1", 1, "L", 2, 2),
    ("r1", 1, "L", 2, 3), ("sb", 0, -1, 0), ("r1", 0, "S", 3, 0), ("r1", 0, "S", 3, 1),
    ("sb", 0, 1, 0), ("sb", 0, 0, 0), ("sb", 1, 0, 0), ("sb", 1, 0, 1),
    ("r1", 1, "S", 1, 0), ("r1", 1, "S", 1, 1), ("r1", 1, "S", 1, 2), ("r1", 1, "S", 1, 3),
    ("r1", 0, "L", 3, 0), ("r1", 1, "L", 1, 0), ("r1", 0, "S", 2, 0), ("r1", 0, "L", 3, 1),
    ("r1", 1, "L", 1, 1), ("r1", 0, "S", 2, 1), ("r1", 1, "L", 1, 2), ("r1", 0, "L", 2, 0),
    ("r1", 1, "L", 1, 3), ("r1", 0, "S", 1, 0), ("r1", 0, "L", 2, 1), ("h1", 1, 0),
    ("r1", 0, "S", 1, 1), ("h1", 1, 1), ("r1", 0, "L", 1, 0), ("h1", 1, 2),
    ("r1", 0, "L", 1, 1), ("h1", 1, 3), ("r2", 1, "L", 4), ("r2", 1, "L", 3),
    ("r2", 1, "S", 3), ("r2", 1, "S", 2), ("h1", 0, 0), ("h1", 0, 1),
    ("r2", 0, "L", 2), ("r2", 0, "L", 1), ("r2", 0, "S", 1), ("r2", 1, "L", 2),
    ("r2", 1, "S", 1), ("r2", 1, "L", 1), ("h2", 0), ("h2", 1),
]


def kernel(
    q_hbm, tags_ref, ans_s, kv_hbm, span_hbm, w_hbm,
    att_ref, small_ref,
    q_ref, span_ref, w_ref, ring_tally, tags_v, idx_v, idx_s,
    g0, g1, kv, sbuf, res, dm, dl, spst, fscr,
    sib_s, sib_ss, sib_r, sib_rs, m1_s, m1_ss, m1_r, m1_rs, m2_s, m2_ss, m2_r, m2_rs,
    r0, r0s, r1, r1s, lg, ta, tz,
    in_sem, ag_send, ag_recv, sg_send, sg_recv,
    sib_send, sib_recv, m1_send, m1_recv, m2_send, m2_recv, tail_send, tail_recv,
):
    dp = lax.axis_index("dp")
    y = lax.axis_index("mp")
    core = dp % 2
    z = (dp // 2) % NZ
    x = dp // (2 * NZ)
    s = 1 - 2 * core
    other = 1 - core

    def device(xx, zz, cc, yy):
        return (xx * (2 * NZ) + zz * 2 + cc, yy)

    def along_x(k):
        return (x + s * k + 2 * NX) % NX

    def along_z(k):
        return (z + s * k + 2 * NZ) % NZ

    sibling = device(x, z, other, y)
    link = {
        "x+": device(along_x(1), z, core, y),
        "x-": device(along_x(-1), z, core, y),
        "z+": device(x, along_z(1), core, y),
        "z-": device(x, along_z(-1), core, y),
        "x++": device(along_x(2), z, core, y),
        "z++": device(x, along_z(2), core, y),
        "z--": device(x, along_z(-2), core, y),
    }
    started = []

    def send(src, dst, ssem, rsem, dev):
        copy = pltpu.make_async_remote_copy(
            src_ref=src, dst_ref=dst, send_sem=ssem, recv_sem=rsem,
            device_id=dev, device_id_type=pl.DeviceIdType.MESH,
        )
        copy.start()
        started.append(copy)

    def arrived(dst, ssem, rsem):
        pltpu.make_async_remote_copy(
            src_ref=dst, dst_ref=dst, send_sem=ssem, recv_sem=rsem,
            device_id=sibling, device_id_type=pl.DeviceIdType.MESH,
        ).wait_recv()

    q_copy = pltpu.make_async_copy(q_hbm, q_ref, in_sem.at[0])
    kv_copy = pltpu.make_async_copy(kv_hbm, kv, in_sem.at[1])
    span_copy = pltpu.make_async_copy(span_hbm, span_ref, in_sem.at[2])
    w_copy = pltpu.make_async_copy(w_hbm, w_ref, in_sem.at[3])
    q_copy.start()
    peers = [sibling]
    peers += [device((x + d) % NX, z, core, y) for d in range(1, NX)]
    peers += [device(x, (z + d) % NZ, core, y) for d in (1, 2, NZ - 2, NZ - 1)]
    peers += [device(x, z, core, (y + d) % NY) for d in range(1, NY)]
    barrier = pltpu.get_barrier_semaphore()
    for peer in peers:
        pl.semaphore_signal(barrier, inc=1, device_id=peer, device_id_type=pl.DeviceIdType.MESH)
    span_copy.start()
    w_copy.start()
    q_copy.wait()
    pl.semaphore_wait(barrier, len(peers))

    gathered = (g0, g1)

    def unit_row(key):
        head, xr, zr = key
        xx, zz = along_x(xr), along_z(zr)
        if head == 0:
            return ((core * NZ + zz) * NX + xx) * 2
        return ((core * NX + xx) * NZ + zz) * 2

    lanes = lax.broadcasted_iota(jnp.int32, (ROWS, 128), 1)

    def query_rows(tile):
        return jnp.concatenate([tile[:, g * 128 : (g + 1) * 128] for g in range(GROUP)], axis=0)

    def as_rows(mat):
        return jnp.concatenate([mat, jnp.zeros((128 - ROWS, 128), F32)], axis=0).T

    square = lax.broadcasted_iota(jnp.int32, (128, 128), 0)

    def tables():
        tags_v[...] = jnp.full((8, 128), -1, jnp.int32)
        for i in range(8):
            tags_v[i : i + 1, 0:SLOTS] = tags_ref[...]
        tag = tags_v[0:1, :]
        down = jnp.concatenate([tags_v[...]] * 16, axis=0).T
        e = lax.broadcasted_iota(jnp.int32, (1, 128), 1)
        b = square
        c, ecore = e % 2, e // 64
        tc, tcore, tz_, tx_ = tag % 2, (tag // 2) % 2, (tag // 4) % NZ, tag // (4 * NZ)
        idx_v[0:1, :] = ((tcore * NZ + tz_) * NX + tx_) * 2 + tc
        idx_v[1:2, :] = ((tcore * NX + tx_) * NZ + tz_) * 2 + tc
        chains = (
            ((((e // 2) % NX) * NZ + (e // 8) % NZ) * 2 + ecore) * 2 + c,
            ((((e // 16) % NX) * NZ + (e // 2) % NZ) * 2 + ecore) * 2 + c,
        )
        for h in range(2):
            hit = down == chains[h]
            idx_v[2 + 2 * h : 3 + 2 * h, :] = jnp.max(jnp.where(hit, EMPTY - b, 0), axis=0, keepdims=True)
            idx_v[3 + 2 * h : 4 + 2 * h, :] = jnp.max(jnp.where(hit, b, -1), axis=0, keepdims=True)
        twin = (down == tag) & (b != e) & (b < SLOTS)
        idx_v[6:7, :] = jnp.max(jnp.where(twin, b, -1), axis=0, keepdims=True)
        idx_v[7:8, :] = e
        copy = pltpu.make_async_copy(idx_v, idx_s, in_sem.at[4])
        copy.start()
        return copy

    def own_spans():
        span_copy.wait()
        keys = lax.broadcasted_iota(jnp.int32, (ROWS, SPAN), 1)
        tokens = lax.broadcasted_iota(jnp.int32, (ROWS, SPAN), 0) % SPAN
        for h in range(2):
            stat = jnp.zeros((ROWS, 128), F32)
            for c in range(2):
                q = query_rows(q_ref[c, :, h * WIDE : (h + 1) * WIDE])
                k = span_ref[c, 0, :, h * 128 : (h + 1) * 128]
                v = span_ref[c, 1, :, h * 128 : (h + 1) * 128]
                sc = lax.dot_general(q, k, (((1,), (1,)), ((), ())), preferred_element_type=F32) * SCALE
                sc = jnp.where(tokens >= keys, sc, big_neg)
                top = jnp.max(sc, axis=1, keepdims=True)
                wt = jnp.exp(sc - top)
                stat = jnp.where(lanes == c, top, stat)
                stat = jnp.where(lanes == 2 + c, jnp.sum(wt, axis=1, keepdims=True), stat)
                res[OWN + c, h] = jnp.dot(wt.astype(BF16), v, preferred_element_type=F32)
            spst[h] = as_rows(stat)[0:8, :]

    count = 0
    done = {}
    for step, key in enumerate(ARRIVALS):
        if step == 2:
            kv_copy.start()
        if step == 8:
            tables_copy = tables()
        if step == 12:
            own_spans()
        head, xr, zr = key
        here = gathered[head].at[pl.ds(unit_row(key), 2)]
        if xr == 0 and zr == 0:
            src = q_ref.at[:, :, pl.ds(head * WIDE, WIDE)]
        else:
            arrived(here, ag_send.at[0], ag_recv.at[UNIT[key]])
            src = here
        for move in onward(key):
            dx, dz = MOVES[move]
            there = UNIT[(head, xr + dx, zr + dz)]
            send(src, here, ag_send.at[count], ag_recv.at[there], link[move])
            count += 1
        if xr == 0 and zr == 0:
            for c in range(2):
                gathered[head][unit_row(key) + c] = q_ref[c, :, head * WIDE : (head + 1) * WIDE]
        bundle = (head, zr if head == 0 else xr)
        done[bundle] = done.get(bundle, 0) + 1
        if head == 0 and done[bundle] == NX:
            zz = along_z(zr)
            rows = g0.at[pl.ds((core * NZ + zz) * NX * 2, NX * 2)]
            send(rows, rows, sg_send.at[zz], sg_recv.at[zz], sibling)
        if head == 1 and done[bundle] == NZ:
            xx = along_x(xr)
            rows = g1.at[pl.ds((core * NX + xx) * NZ * 2, NZ * 2)]
            send(rows, rows, sg_send.at[NZ + xx], sg_recv.at[NZ + xx], sibling)
    tables_copy.wait()
    kv_copy.wait()

    def scores_of(h):
        def score_step(i, top):
            for u in range(UNROLL):
                b = i * UNROLL + u
                q = query_rows(gathered[h][idx_s[h, b]])
                k = kv[b, 0, :, h * 128 : (h + 1) * 128]
                sc = lax.dot_general(q, k, (((1,), (1,)), ((), ())), preferred_element_type=F32) * SCALE
                sbuf[b, h] = sc
                top = jnp.where(lanes == b, jnp.max(sc, axis=1, keepdims=True), top)
            return top

        return lax.fori_loop(0, SLOTS // UNROLL, score_step, jnp.full((ROWS, 128), big_neg, F32))

    for xx in range(NX):
        rows = g1.at[pl.ds((other * NX + xx) * NZ * 2, NZ * 2)]
        arrived(rows, sg_send.at[NZ + xx], sg_recv.at[NZ + xx])
    top1 = scores_of(1)
    for zz in range(NZ):
        rows = g0.at[pl.ds((other * NZ + zz) * NX * 2, NX * 2)]
        arrived(rows, sg_send.at[zz], sg_recv.at[zz])
    tops = (scores_of(0), top1)

    def pick(mat, *wanted):
        hot = sum((square == w).astype(F32) for w in wanted)
        return jnp.dot(mat, hot, precision=lax.Precision.HIGHEST, preferred_element_type=F32)

    twin = idx_v[6:7, :]
    twin = jnp.where(twin < 0, lax.broadcasted_iota(jnp.int32, (1, 128), 1), twin)
    tops = tuple(jnp.maximum(t, pick(t, twin)) for t in tops)

    def weigh_block(b, carry):
        out = []
        for h in range(2):
            top = jnp.sum(jnp.where(lanes == b, tops[h], 0.0), axis=1, keepdims=True)
            wt = jnp.exp(sbuf[b, h] - top)
            out.append(jnp.where(lanes == b, jnp.sum(wt, axis=1, keepdims=True), carry[h]))
            v = kv[b, 1, :, h * 128 : (h + 1) * 128]
            res[b, h] = jnp.dot(wt.astype(BF16), v, preferred_element_type=F32)
        return tuple(out)

    def weigh_step(i, carry):
        for u in range(UNROLL // 2):
            carry = weigh_block(i * (UNROLL // 2) + u, carry)
        return carry

    sums = lax.fori_loop(0, 2 * SLOTS // UNROLL, weigh_step, (jnp.zeros((ROWS, 128), F32),) * 2)

    for h in range(2):
        res[EMPTY, h] = jnp.zeros((ROWS, 128), F32)
        first = EMPTY - idx_v[2 + 2 * h : 3 + 2 * h, :]
        last = idx_v[3 + 2 * h : 4 + 2 * h, :]
        last = jnp.where(last > first, last, EMPTY)
        dm[h] = as_rows(pick(tops[h], first)).reshape(16, 8, 128)
        dl[h] = as_rows(pick(sums[h], first, last)).reshape(16, 8, 128)

    def merge(n, sources, emit, normal=False):
        top = sources[0][1]
        for _, m, _ in sources[1:]:
            top = jnp.maximum(top, m)
        total = None
        for i, (_, m, l) in enumerate(sources):
            f = jnp.exp(m - top)
            fscr[i * n : (i + 1) * n, :] = f
            total = l * f if total is None else total + l * f
        width = len(sources) * n
        if normal:
            fscr[width : width + n, :] = 1.0 / total
            width += n
        width = (width + 7) // 8 * 8
        cols = fscr[0:width, :].T
        for j in range(n):
            acc = None
            for i, (load, _, _) in enumerate(sources):
                term = load(j) * cols[:ROWS, i * n + j : i * n + j + 1]
                acc = term if acc is None else acc + term
            if normal:
                at = len(sources) * n + j
                acc = acc * cols[:ROWS, at : at + 1]
            emit(j, acc)
        return top, total

    def held(h, cc, g, first, n):
        group = cc * 8 + g

        def load(j):
            at = group * 8 + first + j
            one, two = EMPTY - idx_s[2 + 2 * h, at], idx_s[3 + 2 * h, at]
            return res[one, h] + res[jnp.where(two > one, two, EMPTY), h]

        return load, dm[h, group, first : first + n, :], dl[h, group, first : first + n, :]

    def group_at(h, k, half):
        return along_z(k) if h == 0 else along_x(k) * 2 + half

    def to_sibling(h, k, half):
        g = group_at(h, k, half)
        load, m, l = held(h, other, g, 0, 8)
        at = h * 8 + g
        for j in range(8):
            sib_s[at, j] = load(j).astype(BF16)
        sib_ss[at, 0:8, :] = m
        sib_ss[at, 8:16, :] = l
        send(sib_ss.at[at], sib_rs.at[at], sib_send.at[16 + at], sib_recv.at[16 + at], sibling)
        send(sib_s.at[at], sib_r.at[at], sib_send.at[at], sib_recv.at[at], sibling)

    seen = set()

    def from_sibling(h, g, key, first, n):
        at = h * 8 + g
        if key not in seen:
            seen.add(key)
            arrived(sib_rs.at[at], sib_send.at[16 + at], sib_recv.at[16 + at])
            arrived(sib_r.at[at], sib_send.at[at], sib_recv.at[at])
        stat = sib_rs[at, first : first + n, :], sib_rs[at, 8 + first : 8 + first + n, :]
        return (lambda j: sib_r[at, first + j].astype(F32)), *stat

    def from_ring1(key, n):
        at = MSG1[key]
        arrived(m1_rs.at[at, pl.ds(0, 2 * n)], m1_send.at[at, 1], m1_recv.at[at, 1])
        arrived(m1_r.at[at, pl.ds(0, n)], m1_send.at[at, 0], m1_recv.at[at, 0])
        return (lambda j: m1_r[at, j].astype(F32)), m1_rs[at, 0:n, :], m1_rs[at, n : 2 * n, :]

    def from_ring2(key):
        at = MSG2[key]
        arrived(m2_rs.at[at], m2_send.at[at, 1], m2_recv.at[at, 1])
        arrived(m2_r.at[at], m2_send.at[at, 0], m2_recv.at[at, 0])
        return (lambda j: m2_r[at, j].astype(F32)), m2_rs[at, 0:2, :], m2_rs[at, 2:4, :]

    def local(h, k, half):
        block = 0 if h == 0 else half // 2
        g = group_at(h, k, block)
        first, n = (half % 2) * 4, 4
        return n, [held(h, core, g, first, n), from_sibling(h, g, (h, k, block), first, n)]

    def ring1(h, arm, k, half):
        at = MSG1[(h, arm, k, half)]
        n, sources = local(h, k if arm == "L" else -k, half)
        if (h, arm, k + 1, half) in MSG1:
            sources.append(from_ring1((h, arm, k + 1, half), n))

        def emit(j, acc):
            m1_s[at, j] = acc.astype(BF16)

        m, l = merge(n, sources, emit)
        m1_ss[at, 0:n, :] = m
        m1_ss[at, n : 2 * n, :] = l
        dev = link[("z" if h == 0 else "x") + ("+" if arm == "L" else "-")]
        stat, data = pl.ds(0, 2 * n), pl.ds(0, n)
        send(m1_ss.at[at, stat], m1_rs.at[at, stat], m1_send.at[at, 1], m1_recv.at[at, 1], dev)
        send(m1_s.at[at, data], m1_r.at[at, data], m1_send.at[at, 0], m1_recv.at[at, 0], dev)

    def home1(h, half):
        n, sources = local(h, 0, half)
        sources += [from_ring1((h, "L", 1, half), n), from_ring1((h, "S", 1, half), n)]
        acc_ref, stat_ref = (r0, r0s) if h == 0 else (r1, r1s)

        def emit(j, acc):
            acc_ref[half * n + j] = acc

        m, l = merge(n, sources, emit)
        for i in range(n // 2):
            at = half * (n // 2) + i
            stat_ref[at, 0:2, :] = m[2 * i : 2 * i + 2, :]
            stat_ref[at, 2:4, :] = l[2 * i : 2 * i + 2, :]

    def reduced(h, pos):
        acc_ref, stat_ref = (r0, r0s) if h == 0 else (r1, r1s)
        return (lambda j: acc_ref[pos * 2 + j]), stat_ref[pos, 0:2, :], stat_ref[pos, 2:4, :]

    def ring2(h, arm, k):
        at = MSG2[(h, arm, k)]
        move, joins = STAGE2[(h, arm, k)]
        offset = k if arm == "L" else -k
        source = reduced(h, along_x(offset) if h == 0 else along_z(offset))
        if joins is None:
            for j in range(2):
                m2_s[at, j] = source[0](j).astype(BF16)
            m, l = source[1], source[2]
        else:

            def emit(j, acc):
                m2_s[at, j] = acc.astype(BF16)

            m, l = merge(2, [source, from_ring2(joins)], emit)
        m2_ss[at, 0:2, :] = m
        m2_ss[at, 2:4, :] = l
        m2_ss[at, 4:8, :] = jnp.zeros((4, 128), F32)
        send(m2_ss.at[at], m2_rs.at[at], m2_send.at[at, 1], m2_recv.at[at, 1], link[move])
        send(m2_s.at[at], m2_r.at[at], m2_send.at[at, 0], m2_recv.at[at, 0], link[move])

    def home2(h):
        span = (lambda j: res[OWN + j, h]), spst[h, 0:2, :], spst[h, 2:4, :]
        sources = [reduced(h, x if h == 0 else z), span]
        sources += [from_ring2((h, *last)) for last in LAST[h]]

        def emit(j, acc):
            for g in range(GROUP):
                col = h * WIDE + g * 128
                att_ref[j, :, col : col + 128] = acc[g * SPAN : (g + 1) * SPAN, :].astype(BF16)

        merge(2, sources, emit, normal=True)

    run = {"sb": to_sibling, "r1": ring1, "h1": home1, "r2": ring2, "h2": home2}
    for step in STEPS:
        run[step[0]](*step[1:])

    w_copy.wait()
    def bits(ref, src_at, dst_at, sem, dev):
        send(ref.at[src_at], ref.at[dst_at], tail_send.at[sem], tail_recv.at[sem], dev)

    for c in range(2):
        lg[y, c * SPAN : (c + 1) * SPAN, :] = jnp.dot(
            att_ref[c], w_ref[...], preferred_element_type=F32
        )
    for d in range(1, NY):
        bits(lg, y, y, d - 1, device(x, z, core, (y + d) % NY))
    for d in range(1, NY):
        arrived(lg.at[(y + NY - d) % NY], tail_send.at[d - 1], tail_recv.at[d - 1])
    logits = lg[0] + lg[1] + lg[2] + lg[3]
    peak = jnp.max(logits, axis=1, keepdims=True)
    norm = peak + jnp.log(jnp.sum(jnp.exp(logits - peak), axis=1, keepdims=True))
    cand = lax.broadcasted_iota(jnp.int32, (SPAN, NCAND), 1)
    prompt_row = lax.broadcasted_iota(jnp.int32, (8, NCAND), 0)
    cand8 = lax.broadcasted_iota(jnp.int32, (8, NCAND), 1)
    tally = jnp.zeros((8, NCAND), F32)
    scores = []
    for c in range(2):
        rows = slice(c * SPAN, (c + 1) * SPAN)
        chosen = jnp.sum(jnp.where(cand == ans_s[c], logits[rows], 0.0), axis=1, keepdims=True)
        score = jnp.sum(chosen - norm[rows]) * (1.0 / SPAN)
        scores.append(score)
        prompt = (dp * 2 + c) // SAMPLES
        tally = tally + jnp.where((prompt_row == prompt) & (cand8 == ans_s[c]), score, 0.0)
    here = x * 2 + core
    ta[here] = tally
    for d in range(1, 2 * NX):
        dx, dc = d // 2, d % 2
        dev = device((x + dx) % NX, z, (core + dc) % 2, y)
        bits(ta, here, here, 2 + d, dev)
    for d in range(1, 2 * NX):
        dx, dc = d // 2, d % 2
        source = (x + NX - dx) % NX * 2 + (core + dc) % 2
        arrived(ta.at[source], tail_send.at[2 + d], tail_recv.at[2 + d])
    part = ta[0]
    for i in range(1, 2 * NX):
        part = part + ta[i]
    tz[z] = part
    for d in range(1, NZ):
        bits(tz, z, z, 9 + d, device(x, (z + d) % NZ, core, y))
    for d in range(1, NZ):
        arrived(tz.at[(z + NZ - d) % NZ], tail_send.at[9 + d], tail_recv.at[9 + d])
    whole = tz[0]
    for i in range(1, NZ):
        whole = whole + tz[i]
    ring_tally[:, 0:8] = whole.T
    small_ref[0:2, :] = jnp.zeros((2, 128), F32)
    small_ref[0:2, 0:8] = ring_tally[pl.ds(dp * 2, 2), 0:8]
    row = lax.broadcasted_iota(jnp.int32, (2, 128), 0)
    small_ref[2:4, :] = jnp.where(row == 0, scores[0], scores[1])
    small_ref[4:8, :] = jnp.zeros((4, 128), F32)
    for copy in started:
        copy.wait_send()


def hand_out(att_ref, small_ref, out_ref, score_ref, tally_ref):
    out_ref[...] = att_ref[...]
    tally_ref[...] = small_ref[0:2, 0:8]
    score_ref[0] = small_ref[2, 0]
    score_ref[1] = small_ref[3, 0]


def per_device(queries, key_value_cache, slot_tags, span_key_value, answer_id, w_cand):
    vmem = pl.BlockSpec(memory_space=pltpu.VMEM)
    smem = pl.BlockSpec(memory_space=pltpu.SMEM)
    anywhere = pl.BlockSpec(memory_space=pl.ANY)
    unit = (8, ROWS, 128)
    stat = (16, 128)
    dma = pltpu.SemaphoreType.DMA
    n1, n2 = len(STAGE1), len(STAGE2)
    sends = sum(len(onward(key)) for key in ARRIVALS)
    attended, small = pl.pallas_call(
        kernel,
        out_shape=(
            jax.ShapeDtypeStruct((2, SPAN, 2 * WIDE), BF16),
            jax.ShapeDtypeStruct((8, 128), F32),
        ),
        in_specs=[anywhere, vmem, smem, anywhere, anywhere, anywhere],
        out_specs=(vmem, vmem),
        scratch_shapes=[
            pltpu.VMEM(queries.shape, BF16),
            pltpu.VMEM(span_key_value.shape, BF16),
            pltpu.VMEM(w_cand.shape, BF16),
            pltpu.VMEM((128, 128), F32),
            pltpu.VMEM((8, 128), jnp.int32),
            pltpu.VMEM((8, 128), jnp.int32),
            pltpu.SMEM((8, 128), jnp.int32),
            pltpu.VMEM((128, SPAN, WIDE), BF16),
            pltpu.VMEM((128, SPAN, WIDE), BF16),
            pltpu.VMEM(key_value_cache.shape, BF16),
            pltpu.VMEM((SLOTS, 2, ROWS, 128), F32),
            pltpu.VMEM((SLOTS + 3, 2, ROWS, 128), F32),
            pltpu.VMEM((2, 16, 8, 128), F32),
            pltpu.VMEM((2, 16, 8, 128), F32),
            pltpu.VMEM((2, 8, 128), F32),
            pltpu.VMEM((128, 128), F32),
            pltpu.VMEM((16, *unit), BF16),
            pltpu.VMEM((16, *stat), F32),
            pltpu.VMEM((16, *unit), BF16),
            pltpu.VMEM((16, *stat), F32),
            pltpu.VMEM((n1, 4, ROWS, 128), BF16),
            pltpu.VMEM((n1, 8, 128), F32),
            pltpu.VMEM((n1, 4, ROWS, 128), BF16),
            pltpu.VMEM((n1, 8, 128), F32),
            pltpu.VMEM((n2, 2, ROWS, 128), BF16),
            pltpu.VMEM((n2, 8, 128), F32),
            pltpu.VMEM((n2, 2, ROWS, 128), BF16),
            pltpu.VMEM((n2, 8, 128), F32),
            pltpu.VMEM((8, ROWS, 128), F32),
            pltpu.VMEM((4, 8, 128), F32),
            pltpu.VMEM((16, ROWS, 128), F32),
            pltpu.VMEM((8, 8, 128), F32),
            pltpu.VMEM((NY, 2 * SPAN, NCAND), F32),
            pltpu.VMEM((2 * NX, 8, 128), F32),
            pltpu.VMEM((NZ, 8, 128), F32),
            dma((5,)),
            dma((sends,)), dma((len(ARRIVALS),)), dma((NZ + NX,)), dma((NZ + NX,)),
            dma((32,)), dma((32,)), dma((n1, 2)), dma((n1, 2)), dma((n2, 2)), dma((n2, 2)),
            dma((17,)), dma((17,)),
        ],
        compiler_params=pltpu.CompilerParams(
            collective_id=0, has_side_effects=True, vmem_limit_bytes=60 * 1024 * 1024
        ),
        name="score_chains",
    )(queries, slot_tags[None], answer_id, key_value_cache, span_key_value, w_cand)
    attended, score, tally = pl.pallas_call(
        hand_out,
        out_shape=(
            jax.ShapeDtypeStruct(attended.shape, BF16),
            jax.ShapeDtypeStruct((2,), F32),
            jax.ShapeDtypeStruct((2, 8), F32),
        ),
        in_specs=[vmem, vmem],
        out_specs=(vmem, smem, vmem),
        name="hand_out",
    )(attended, small)
    return attended, score, tally.T


def solution(mesh):
    in_specs = (
        P("dp", None, "mp"),
        P("dp", None, None, "mp"),
        P("dp"),
        P("dp", None, None, "mp"),
        P("dp"),
        P("mp", None),
    )
    out_specs = (P("dp", None, "mp"), P("dp"), P(None, "dp"))
    return jax.shard_map(
        per_device, mesh=mesh, in_specs=in_specs, out_specs=out_specs, check_vma=False
    )
```
